32 devices in a mesh: slab: 8 (over y, x, core), tile: 4 (over z).
Axes of the slice: x: 2, y: 2, z: 4, core: 2. Of those that a mesh axis runs over, the one named last changes fastest.
Arguments:
- volume: float32 [128, 256, 1024], P('slab', 'tile'), may hold values from -0.3 to 0.3
- shears: float32 [8], replicated, may hold values from -0.4 to 0.4
- tile_shift: int32 [8, 4], P(None, 'tile'), may hold values from -1 to 1
- illumination: float32 [2, 128, 128], replicated, may hold values from -6 to 6
- measured: bfloat16 [1024, 128, 128], P(('slab', 'tile')), may hold values from 0.049804688 to 2.5
- frame_owner: int32 [1024, 1], P(('slab', 'tile')), may hold values from 0 to 7; in each aligned block of 32 rows (0 to 31, 32 to 63, ...) at most 8 rows name the same one
- frame_shift: int32 [1024], P(('slab', 'tile')), may hold values from -32 to 160
Outputs:
- volume_grad: float32 [128, 256, 1024], P('slab', 'tile')
The draws below stay inside these ranges and needn't reach their ends.
Inputs may be any that keep to these rules, and one draw needn't show every extreme that they name: `frame_owner`: the 32 frames of one device name each angle at most 8 times, a bound that some block reaches.
All inputs are finite; a program needn't handle non-finite values.
Results may differ from the reference program's by a relative error of at most 0.012.
Values may be sent and summed in bfloat16 or wider, within the bound.
A program may use at most 256 MiB of HBM per device.

```python
import math
import jax
import jax.numpy as jnp
import numpy as np
from jax import lax

SIDE = 128
SLICES = 128
GRID = 1024
BLOCK = 128
HALO = 32
ZT_DEV = 64
FR_DEV = 32
NZ = 256
ANGLES = 8
NFR = 1024
CAP = 8
N_SLAB = 8
N_TILE = 4


def set_ends(values, key, least, top_value):
    longest = values.shape.index(max(values.shape))
    spots = []
    for shift in (0, 1):
        where = [jax.random.randint(jax.random.fold_in(key, axis), (), 0, length) for axis, length in enumerate(values.shape)]
        where[longest] = (where[longest] + shift) % values.shape[longest]
        spots.append(tuple(where))
    return values.at[spots[0]].set(least).at[spots[1]].set(top_value)


def levels(key, extent, shards, smallest, high):
    def one(dim, blocks):
        draws = jax.random.uniform(jax.random.fold_in(jax.random.fold_in(key, 6), dim), (blocks,), jnp.float32, smallest / len(shards), high / len(shards))
        return jnp.repeat(jnp.exp(draws), extent[dim] // blocks).reshape((-1,) + (1,) * (len(extent) - dim - 1))

    gain = one(*shards[0])
    for cut in shards[1:]:
        gain = gain * one(*cut)
    return gain


def assign_block(stream_key, own, number, rows, count, top, reach, slope):
    order = jax.random.permutation(stream_key, count)
    heavy_load, usual = shares(count, rows * top, reach, slope, True), shares(count, rows * top, reach, slope, False)
    places = jnp.arange(count)

    def named(tallies, turn):
        used = int((tallies > 0).sum())
        fixed = max(1, used // 4)
        moved = fixed + (places - fixed + turn * (used - fixed)) % max(1, count - fixed)
        return jnp.zeros((count,), jnp.int32).at[order[jnp.where(places < fixed, places, moved)]].set(jnp.asarray(tallies, jnp.int32))

    tallies = jnp.where(number % 4 == 0, named(heavy_load, number // 4), named(usual, number - number // 4 - 1))
    mixed = jax.random.permutation(jax.random.fold_in(own, 3), count)
    source_of, taker = mixed[0:count // 2 * 2:2], mixed[1:count // 2 * 2:2]
    room = jnp.minimum(tallies[source_of] - 1, reach - tallies[taker]) // 2
    room = jnp.where((source_of == order[0]) | (taker == order[0]) | (tallies[taker] == 0), 0, jnp.maximum(room, 0))
    moved = jax.random.randint(jax.random.fold_in(own, 4), (count // 2,), 0, 1 << 20) % (room + 1)
    tallies = tallies.at[source_of].add(-moved).at[taker].add(moved)
    items = jnp.searchsorted(jnp.cumsum(tallies), jnp.arange(rows * top), side="right").astype(jnp.int32)
    grid = items.reshape(top, rows).T
    grid = grid[jax.random.permutation(jax.random.fold_in(own, 1), rows)]
    turn = jax.random.randint(jax.random.fold_in(own, 2), (rows, 1), 0, top)
    return jnp.take_along_axis(grid, (jnp.arange(top)[None, :] + turn) % top, axis=1)


def shares(amount, total, bound, lean, full):
    portions = [(1 << 20) // math.isqrt(rank ** lean) + 1 for rank in range(1, amount + 1)]
    largest = bound if full else min(bound, max(-(-total // amount), total * portions[0] // sum(portions)))
    least = 1 if total - largest >= amount - 1 else 0
    holding, rest = [largest] + [least] * (amount - 1), total - largest - least * (amount - 1)
    while rest > 0:
        free = [i for i in range(1, amount) if holding[i] < largest] or [i for i in range(1, amount) if holding[i] < bound]
        pool, left = sum([portions[i] for i in free]), rest
        for i in free:
            more = min(bound - holding[i], max(1, left * portions[i] // pool), rest)
            holding[i] = holding[i] + more
            rest = rest - more
    return np.array(holding)


def bell_draw(stream_key, extent, width, bound, split=(), kind=jnp.bfloat16):
    entries = jax.random.normal(stream_key, extent, jnp.float32) * width
    if len(split) > 0:
        entries = levels(stream_key, extent, split, -0.22, 0.18) * entries
    return jnp.clip(entries, min=-bound, max=bound).astype(kind)


def setup_inputs(seed: int = 0) -> dict:
    splits = jax.random.split(jax.random.key(seed), 8)
    volume = bell_draw(splits[0], (SLICES, NZ, GRID), 0.05, 0.3, ((0, 8), (1, 4)), jnp.float32)
    shears = jnp.clip(jax.random.uniform(splits[1], (ANGLES,), jnp.float32, -0.4, 0.4), -0.4, 0.4)
    tile_shift = set_ends(jax.random.randint(splits[2], (ANGLES, N_TILE), -1, 2), jax.random.fold_in(splits[2], 1), -1, 1).astype(jnp.int32)
    illumination = bell_draw(splits[3], (2, SIDE, SIDE), 1.0, 6.0, (), jnp.float32)
    measured = jnp.clip(0.049804688 + 2.4501953 * jax.random.uniform(splits[4], (NFR, SIDE, SIDE), jnp.float32) ** levels(splits[4], (NFR, SIDE, SIDE), ((0, 32),), -0.2, 0.2), 0.049804688, 2.5).astype(jnp.bfloat16)
    frame_owner_keys = jax.random.split(jax.random.fold_in(splits[5], 1), NFR // FR_DEV)
    frame_owner_turns = jax.random.permutation(jax.random.fold_in(splits[5], 3), NFR // FR_DEV)
    frame_owner = jax.vmap(lambda own, number: assign_block(jax.random.fold_in(splits[5], 2), own, number, FR_DEV, N_SLAB, 1, CAP, 2))(frame_owner_keys, frame_owner_turns).reshape((NFR, 1))
    frame_shift = set_ends(jax.random.randint(splits[6], (NFR,), -HALO, GRID // N_TILE - SIDE + HALO + 1), jax.random.fold_in(splits[6], 1), -HALO, (GRID // N_TILE - SIDE + HALO + 1) - 1).astype(jnp.int32)
    return dict(volume=volume, shears=shears, tile_shift=tile_shift, illumination=illumination, measured=measured, frame_owner=frame_owner, frame_shift=frame_shift)


smoothing = 0.25
highest = lax.Precision.HIGHEST

def beam_kernel(shear_one, beam_depth, block_width):
    beam_pos = jnp.arange(beam_depth, dtype=jnp.float32)
    centre = block_width * 0.5 + (beam_pos - (beam_depth - 1) * 0.5) * shear_one
    source = jnp.arange(block_width, dtype=jnp.float32)
    target = jnp.arange(2 * block_width, dtype=jnp.float32)
    spread = target[None, None, :] - source[None, :, None] - centre[:, None, None]
    values = jnp.exp(-0.5 * spread * spread).astype(jnp.bfloat16)
    return values.reshape(beam_depth * block_width, 2 * block_width)

def dft_tables(length):
    indices = jnp.arange(length, dtype=jnp.int32)
    product = indices[:, None] * indices[None, :] % length
    phases = product.astype(jnp.float32) * (2.0 * math.pi / length)
    return (jnp.cos(phases), jnp.sin(phases))

def left_mul(matrix, frames_in):
    return jnp.einsum('jk,nkl->njl', matrix, frames_in, precision=highest)

def right_mul(frames_in, matrix):
    return jnp.einsum('njk,kl->njl', frames_in, matrix, precision=highest)

def phase_gradient(windows, illumination, amplitude, dft_cos, dft_sin):
    length = dft_cos.shape[0]
    object_re = jnp.cos(windows)
    object_im = jnp.sin(windows)
    probe_re = illumination[0]
    probe_im = illumination[1]
    wave_re = probe_re * object_re - probe_im * object_im
    wave_im = probe_re * object_im + probe_im * object_re
    half_re = left_mul(dft_cos, wave_re) + left_mul(dft_sin, wave_im)
    half_im = left_mul(dft_cos, wave_im) - left_mul(dft_sin, wave_re)
    far_re = (right_mul(half_re, dft_cos) + right_mul(half_im, dft_sin)) / length
    far_im = (right_mul(half_im, dft_cos) - right_mul(half_re, dft_sin)) / length
    modulus = jnp.sqrt(far_re * far_re + far_im * far_im + smoothing)
    factor = 1.0 - amplitude / modulus
    resid_re = far_re * factor
    resid_im = far_im * factor
    back_re = left_mul(dft_cos, resid_re) - left_mul(dft_sin, resid_im)
    back_im = left_mul(dft_cos, resid_im) + left_mul(dft_sin, resid_re)
    near_re = (right_mul(back_re, dft_cos) - right_mul(back_im, dft_sin)) / length
    near_im = (right_mul(back_im, dft_cos) + right_mul(back_re, dft_sin)) / length
    grad_re = probe_re * near_re + probe_im * near_im
    grad_im = probe_re * near_im - probe_im * near_re
    return grad_im * object_re - grad_re * object_im

def reference(volume, shears, tile_shift, illumination, measured, frame_owner, frame_shift):
    blocks_row = GRID // BLOCK
    own_width = GRID // N_TILE
    block_ids = jnp.arange(blocks_row, dtype=jnp.int32)
    volume_half = lax.optimization_barrier(volume.astype(jnp.bfloat16))

    def make_kernel(shear_one):
        return beam_kernel(shear_one, ZT_DEV, BLOCK)
    kernels = lax.optimization_barrier(lax.map(make_kernel, shears))

    def selector(offset, plus_one):
        return (block_ids[:, None] == block_ids[None, :] + offset + plus_one).astype(jnp.float32)

    def project_angle(angle_id):
        kernel_wide = kernels[angle_id].astype(jnp.float32)

        def per_tile(running, tile_id):
            part_volume = lax.dynamic_slice_in_dim(volume_half, tile_id * ZT_DEV, ZT_DEV, 1)
            rows_matrix = part_volume.reshape(SLICES, ZT_DEV, blocks_row, BLOCK).transpose(0, 2, 1, 3)
            rows_matrix = rows_matrix.reshape(SLICES * blocks_row, ZT_DEV * BLOCK).astype(jnp.float32)
            partial_sum = jnp.dot(rows_matrix, kernel_wide, precision=highest).reshape(SLICES, blocks_row, 2, BLOCK)
            offset = tile_shift[angle_id, tile_id]
            shifted = jnp.einsum('ki,sib->skb', selector(offset, 0), partial_sum[:, :, 0], precision=highest)
            shifted = shifted + jnp.einsum('ki,sib->skb', selector(offset, 1), partial_sum[:, :, 1], precision=highest)
            return (running + shifted, None)
        initial = jnp.zeros((SLICES, blocks_row, BLOCK), jnp.float32)
        running, unused = lax.scan(per_tile, initial, jnp.arange(N_TILE, dtype=jnp.int32))
        return running.reshape(SLICES, GRID)
    projection = lax.map(project_angle, jnp.arange(ANGLES, dtype=jnp.int32))
    phase_pad = jnp.pad(projection, ((0, 0), (0, 0), (HALO, HALO)))
    dft_cos, dft_sin = dft_tables(SIDE)
    frame_ids = jnp.arange(NFR, dtype=jnp.int32)
    starts = frame_ids // FR_DEV % N_TILE * own_width + frame_shift + HALO
    angles = frame_owner[:, 0]
    batches = NFR // FR_DEV
    zero_index = jnp.zeros((), jnp.int32)

    def one_batch(grad_pad, batch_data):
        angle_batch, start_batch, amp_batch = batch_data

        def cut_one(angle_id, start_col):
            return lax.dynamic_slice(phase_pad[angle_id], (zero_index, start_col), (SIDE, SIDE))
        windows = jax.vmap(cut_one)(angle_batch, start_batch)
        dphase = phase_gradient(windows, illumination, amp_batch.astype(jnp.float32), dft_cos, dft_sin)

        def add_one(member, current):
            corner = (angle_batch[member], zero_index, start_batch[member])
            current_piece = lax.dynamic_slice(current, corner, (1, SIDE, SIDE))
            return lax.dynamic_update_slice(current, current_piece + dphase[member][None], corner)
        return (lax.fori_loop(0, FR_DEV, add_one, grad_pad), None)
    grad_initial = jnp.zeros_like(phase_pad)
    batch_inputs = (angles.reshape(batches, FR_DEV), starts.reshape(batches, FR_DEV), measured.reshape(batches, FR_DEV, SIDE, SIDE))
    grad_pad, unused = lax.scan(one_batch, grad_initial, batch_inputs)
    proj_grad = lax.optimization_barrier(grad_pad[:, :, HALO:HALO + GRID].astype(jnp.bfloat16))
    proj_wide = proj_grad.astype(jnp.float32).reshape(ANGLES, SLICES, blocks_row, BLOCK)

    def back_tile(tile_id):

        def per_angle(running, angle_id):
            kernel_wide = kernels[angle_id].astype(jnp.float32)
            offset = tile_shift[angle_id, tile_id]
            grad_rows = proj_wide[angle_id]
            pick_low = jnp.einsum('ki,skb->sib', selector(offset, 0), grad_rows, precision=highest)
            pick_high = jnp.einsum('ki,skb->sib', selector(offset, 1), grad_rows, precision=highest)
            stacked = jnp.concatenate([pick_low, pick_high], axis=2).reshape(SLICES * blocks_row, 2 * BLOCK)
            return (running + jnp.dot(stacked, kernel_wide.T, precision=highest), None)
        initial = jnp.zeros((SLICES * blocks_row, ZT_DEV * BLOCK), jnp.float32)
        running, unused = lax.scan(per_angle, initial, jnp.arange(ANGLES, dtype=jnp.int32))
        return running.reshape(SLICES, blocks_row, ZT_DEV, BLOCK).transpose(0, 2, 1, 3).reshape(SLICES, ZT_DEV, GRID)
    tile_grads = lax.map(back_tile, jnp.arange(N_TILE, dtype=jnp.int32))
    return tile_grads.transpose(1, 0, 2, 3).reshape(SLICES, NZ, GRID)
```

```python
import functools
import math

import jax
import jax.numpy as jnp
from jax import lax
from jax.experimental import pallas as pl
from jax.experimental.pallas import tpu as pltpu
from jax.sharding import PartitionSpec as P

LANES = 128
HALF = LANES // 2
HALO = 32
SMOOTHING = 0.25
WIRE = jnp.bfloat16
F32 = jnp.float32
BF16 = jnp.bfloat16
MESH = pl.DeviceIdType.MESH
ROOT = math.sqrt(0.5 * math.log2(math.e))
GROUP = 8
SIN_POLY = (3.1415926401307073, -5.1677100835078775, 2.550077523214199, -0.5982912856179897, 0.07765766030124945)
COS_POLY = (0.9999999532476078, -4.934792830619626, 4.0584113528622625, -1.331876568078962, 0.2196896110945085)


def lane_ids(shape):
    return lax.broadcasted_iota(jnp.int32, shape, len(shape) - 1)


def row_ids(shape):
    return lax.broadcasted_iota(jnp.int32, shape, len(shape) - 2)


def halo_join(low, high):
    lanes = lane_ids(low.shape)
    outer = (lanes < HALO) | (lanes >= LANES - HALO)
    return jnp.where(outer, low, pltpu.roll(high, HALF, 1))


def project_kernel(tiles, slices, beams, blocks, shears_ref, shift_ref, v_ref, out_ref, lhs, ker, res, comb):
    angles = shears_ref.shape[0]
    pairs = angles // 2
    own = blocks // tiles
    groups = beams // 8
    half_rows = slices * blocks

    def arrange(group, carried):
        for pair in range(4):
            col = pl.multiple_of((group * 4 + pair) * LANES, LANES)
            for duo in range(slices // 2):
                lower, upper = [], []
                for s in (2 * duo, 2 * duo + 1):
                    start = (s * groups + group) * (blocks * 8) + 2 * pair
                    first = v_ref[pl.ds(start, blocks, stride=8), :]
                    second = v_ref[pl.ds(start + 1, blocks, stride=8), :]
                    left = lane_ids(first.shape) < HALF
                    crossed = pltpu.roll(jnp.where(left, second, first), HALF, 1)
                    lower.append(jnp.where(left, first, crossed))
                    upper.append(jnp.where(left, crossed, second))
                row = 2 * duo * blocks
                lhs[row : row + 2 * blocks, pl.ds(col, LANES)] = jnp.concatenate(lower, 0).astype(BF16)
                row += half_rows
                lhs[row : row + 2 * blocks, pl.ds(col, LANES)] = jnp.concatenate(upper, 0).astype(BF16)
        return carried

    lax.fori_loop(0, groups, arrange, 0)
    shape = (HALF, LANES)
    base = (lane_ids(shape) - row_ids(shape) - HALO).astype(F32) * ROOT
    lanes = lane_ids((half_rows, LANES))
    lanes_s = lane_ids((slices, LANES))

    for p in range(pairs):
        steps = [shears_ref[p] * ROOT, shears_ref[p + pairs] * ROOT]

        def beam(q, carried):
            place = q.astype(F32) - (beams - 1) * 0.5
            row = pl.multiple_of(q * HALF, HALF)
            for side in range(2):
                gap = base - place * steps[side]
                ker[pl.ds(row, HALF), side * LANES : (side + 1) * LANES] = jnp.exp2(-(gap * gap)).astype(BF16)
            return carried

        lax.fori_loop(0, beams, beam, 0, unroll=8)
        res[...] = jnp.dot(lhs[...], ker[...], preferred_element_type=F32)
        sums = []
        for side in range(2):
            cols = slice(side * LANES, (side + 1) * LANES)
            near = pltpu.roll(res[0:half_rows, cols], HALO, 1)
            far = pltpu.roll(res[half_rows : 2 * half_rows, cols], HALO + HALF, 1)
            comb[0] = jnp.where(lanes >= HALO, near, 0.0) + jnp.where(lanes >= HALO + HALF, far, 0.0)
            comb[1] = jnp.where(lanes < HALO, near, 0.0) + jnp.where(lanes < HALO + HALF, far, 0.0)
            shift = shift_ref[p + side * pairs, 0]
            row_of = []
            for k in range(blocks):
                total = jnp.zeros((slices, LANES), F32)
                for o in range(2):
                    i = k - shift - o
                    inside = (i >= 0) & (i < blocks)
                    picked = comb[o, pl.ds(jnp.clip(i, 0, blocks - 1), slices, stride=blocks), :]
                    total += jnp.where(inside, picked, 0.0)
                row_of.append(total)
            sums.append(row_of)
        zero = jnp.zeros((slices, LANES), F32)
        for t in range(tiles):
            margins = []
            for side in range(2):
                for b in range(own):
                    out_ref[t, p, side * own + b] = sums[side][t * own + b].astype(WIRE)
                after = sums[side][(t + 1) * own] if t + 1 < tiles else zero
                before = sums[side][t * own - 1] if t > 0 else zero
                margins.append(jnp.where(lanes_s < HALF, after, before))
            out_ref[t, p, 2 * own] = halo_join(margins[0], margins[1]).astype(WIRE)


def project(shears, tile_shift, volume, tiles):
    slices, beams, width = volume.shape
    blocks = width // LANES
    angles = shears.shape[0]
    own = blocks // tiles
    view = volume.reshape(slices, beams // 8, 8, blocks, LANES).transpose(0, 1, 3, 2, 4).reshape(-1, LANES)
    rows = 2 * slices * blocks
    return pl.pallas_call(
        functools.partial(project_kernel, tiles, slices, beams, blocks),
        out_shape=jax.ShapeDtypeStruct((tiles, angles // 2, 2 * own + 1, slices, LANES), WIRE),
        in_specs=[
            pl.BlockSpec(memory_space=pltpu.SMEM),
            pl.BlockSpec(memory_space=pltpu.SMEM),
            pl.BlockSpec(memory_space=pltpu.VMEM),
        ],
        out_specs=pl.BlockSpec(memory_space=pltpu.VMEM),
        scratch_shapes=[
            pltpu.VMEM((rows, beams * HALF), BF16),
            pltpu.VMEM((beams * HALF, 2 * LANES), BF16),
            pltpu.VMEM((rows, 2 * LANES), F32),
            pltpu.VMEM((2, rows // 2, LANES), F32),
        ],
        compiler_params=pltpu.CompilerParams(vmem_limit_bytes=40 * 1024 * 1024),
        name="project",
    )(shears, tile_shift, view)


def greet(axes):
    barrier = pltpu.get_barrier_semaphore()
    total = 0
    for axis, count in axes:
        me = lax.axis_index(axis)
        for step in range(1, count):
            pl.semaphore_signal(
                barrier, inc=1, device_id={axis: lax.rem(me + step, count)}, device_id_type=MESH
            )
            total += 1
    pl.semaphore_wait(barrier, total)


def phase_exchange_kernel(tiles, slabs, part_ref, phase_ref, came, tile_send, tile_recv, slab_send, slab_recv):
    pairs = part_ref.shape[1]
    slices = part_ref.shape[3]
    me_t = lax.axis_index("tile")
    me_s = lax.axis_index("slab")
    greet((("tile", tiles), ("slab", slabs)))
    rows = pl.ds(pl.multiple_of(me_s * slices, slices), slices)

    def tile_copy(p, step):
        peer = lax.rem(me_t + step, tiles)
        return pltpu.make_async_remote_copy(
            src_ref=part_ref.at[peer, p],
            dst_ref=came.at[step - 1, p],
            send_sem=tile_send.at[step - 1, p],
            recv_sem=tile_recv.at[step - 1, p],
            device_id={"tile": peer},
            device_id_type=MESH,
        )

    def slab_copy(p, step):
        return pltpu.make_async_remote_copy(
            src_ref=phase_ref.at[p, :, rows, :],
            dst_ref=phase_ref.at[p, :, rows, :],
            send_sem=slab_send.at[step - 1, p],
            recv_sem=slab_recv.at[step - 1, p],
            device_id={"slab": lax.rem(me_s + step, slabs)},
            device_id_type=MESH,
        )

    for p in range(pairs):
        for step in range(1, tiles):
            tile_copy(p, step).start()
    for p in range(pairs):
        total = part_ref[me_t, p].astype(F32)
        for step in range(1, tiles):
            tile_copy(p, step).wait_recv()
            total += came[step - 1, p].astype(F32)
        phase_ref[p, :, rows, :] = total.astype(WIRE)
        for step in range(1, slabs):
            slab_copy(p, step).start()
    for p in range(pairs):
        for step in range(1, slabs):
            slab_copy(p, step).wait_recv()
    for p in range(pairs):
        for step in range(1, tiles):
            tile_copy(p, step).wait_send()
        for step in range(1, slabs):
            slab_copy(p, step).wait_send()


def phase_exchange(parts, tiles, slabs):
    pairs, pieces, slices = parts.shape[1:4]
    return pl.pallas_call(
        functools.partial(phase_exchange_kernel, tiles, slabs),
        out_shape=jax.ShapeDtypeStruct((pairs, pieces, slabs * slices, LANES), WIRE),
        in_specs=[pl.BlockSpec(memory_space=pltpu.VMEM)],
        out_specs=pl.BlockSpec(memory_space=pltpu.VMEM),
        scratch_shapes=[
            pltpu.VMEM((tiles - 1, pairs, pieces, slices, LANES), WIRE),
            pltpu.SemaphoreType.DMA((tiles - 1, pairs)),
            pltpu.SemaphoreType.DMA((tiles - 1, pairs)),
            pltpu.SemaphoreType.DMA((slabs - 1, pairs)),
            pltpu.SemaphoreType.DMA((slabs - 1, pairs)),
        ],
        compiler_params=pltpu.CompilerParams(
            collective_id=0, has_side_effects=True, vmem_limit_bytes=16 * 1024 * 1024
        ),
        name="phase_exchange",
    )(parts)


def grad_exchange_kernel(tiles, slabs, grad_ref, out_ref, came, slab_send, slab_recv, tile_send, tile_recv):
    pairs = grad_ref.shape[0]
    slices = out_ref.shape[3]
    me_t = lax.axis_index("tile")
    me_s = lax.axis_index("slab")
    greet((("tile", tiles), ("slab", slabs)))

    def rows_of(slab):
        return pl.ds(pl.multiple_of(slab * slices, slices), slices)

    def slab_copy(p, step):
        peer = lax.rem(me_s + step, slabs)
        return pltpu.make_async_remote_copy(
            src_ref=grad_ref.at[p, :, rows_of(peer), :],
            dst_ref=came.at[step - 1, p],
            send_sem=slab_send.at[step - 1, p],
            recv_sem=slab_recv.at[step - 1, p],
            device_id={"slab": peer},
            device_id_type=MESH,
        )

    def tile_copy(p, step):
        return pltpu.make_async_remote_copy(
            src_ref=out_ref.at[me_t, p],
            dst_ref=out_ref.at[me_t, p],
            send_sem=tile_send.at[step - 1, p],
            recv_sem=tile_recv.at[step - 1, p],
            device_id={"tile": lax.rem(me_t + step, tiles)},
            device_id_type=MESH,
        )

    for p in range(pairs):
        for step in range(1, slabs):
            slab_copy(p, step).start()
    for p in range(pairs):
        total = grad_ref[p, :, rows_of(me_s), :].astype(F32)
        for step in range(1, slabs):
            slab_copy(p, step).wait_recv()
            total += came[step - 1, p].astype(F32)
        out_ref[me_t, p] = total.astype(WIRE)
        for step in range(1, tiles):
            tile_copy(p, step).start()
    for p in range(pairs):
        for step in range(1, tiles):
            tile_copy(p, step).wait_recv()
    for p in range(pairs):
        for step in range(1, tiles):
            tile_copy(p, step).wait_send()
        for step in range(1, slabs):
            slab_copy(p, step).wait_send()


def grad_exchange(grads, tiles, slabs):
    pairs, pieces, all_rows = grads.shape[:3]
    slices = all_rows // slabs
    return pl.pallas_call(
        functools.partial(grad_exchange_kernel, tiles, slabs),
        out_shape=jax.ShapeDtypeStruct((tiles, pairs, pieces, slices, LANES), WIRE),
        in_specs=[pl.BlockSpec(memory_space=pltpu.VMEM)],
        out_specs=pl.BlockSpec(memory_space=pltpu.VMEM),
        scratch_shapes=[
            pltpu.VMEM((slabs - 1, pairs, pieces, slices, LANES), WIRE),
            pltpu.SemaphoreType.DMA((slabs - 1, pairs)),
            pltpu.SemaphoreType.DMA((slabs - 1, pairs)),
            pltpu.SemaphoreType.DMA((tiles - 1, pairs)),
            pltpu.SemaphoreType.DMA((tiles - 1, pairs)),
        ],
        compiler_params=pltpu.CompilerParams(
            collective_id=1, has_side_effects=True, vmem_limit_bytes=16 * 1024 * 1024
        ),
        name="grad_exchange",
    )(grads)


def sin_cos(phase):
    turns = phase * (0.5 / math.pi)
    turns = turns - jnp.round(turns)
    square = turns * turns
    sine, cosine = SIN_POLY[-1], COS_POLY[-1]
    for low_s, low_c in zip(SIN_POLY[-2::-1], COS_POLY[-2::-1]):
        sine = sine * square + low_s
        cosine = cosine * square + low_c
    sine = sine * turns
    double = sine + sine
    return double * cosine, 1.0 - double * sine


def frame_kernel(
    own, owner_ref, start_ref, phase_ref, probe_ref, measured_ref,
    right_ref, left_ref, left_back_ref, right_back_ref, out_ref, acc,
):
    pairs = phase_ref.shape[0]
    frames, side, unused = measured_ref.shape
    ring = own + 1
    acc[...] = jnp.zeros_like(acc)
    lanes = lane_ids((side, LANES))

    def place(member):
        angle = owner_ref[member, 0]
        start = start_ref[member]
        start = jnp.where(start < 0, start + ring * LANES, start)
        first = start // LANES
        offset = start - first * LANES
        second = jnp.where(first + 1 == ring, 0, first + 1)
        return angle, first, second, offset

    def piece(angle, block, offset):
        upper = jnp.where(angle >= pairs, 1, 0)
        pair = angle - upper * pairs
        margin = block == own
        index = jnp.where(margin, 2 * own, upper * own + block)
        turn = jnp.where(margin, upper * HALF, 0) + LANES - offset
        turn = jnp.where(turn >= LANES, turn - LANES, turn)
        return pltpu.roll(phase_ref[pair, index].astype(F32), turn, 1)

    def step(number, carried):
        for duo in range(GROUP // 2):
            two = [number * GROUP + 2 * duo, number * GROUP + 2 * duo + 1]
            waves = []
            for member in two:
                angle, first, second, offset = place(member)
                window = jnp.where(
                    lanes < LANES - offset, piece(angle, first, offset), piece(angle, second, offset)
                )
                sine, cosine = sin_cos(window)
                probe_re, probe_im = probe_ref[0], probe_ref[1]
                waves.append((probe_re * cosine - probe_im * sine, probe_re * sine + probe_im * cosine))
            stacked = jnp.concatenate(
                [jnp.concatenate([re.astype(BF16), im.astype(BF16)], axis=1) for re, im in waves], axis=0
            )
            half = jnp.dot(stacked, right_ref[...], preferred_element_type=F32).astype(BF16)

            def by_lane(value):
                return jnp.concatenate(
                    [
                        jnp.concatenate([value[:side, :LANES], value[side:, :LANES]], axis=1),
                        jnp.concatenate([value[:side, LANES:], value[side:, LANES:]], axis=1),
                    ],
                    axis=0,
                )

            far = jnp.dot(left_ref[...], by_lane(half), preferred_element_type=F32)
            far_re, far_im = far[:side], far[side:]
            amplitude = jnp.concatenate([measured_ref[member] for member in two], axis=1).astype(F32)
            factor = 1.0 - amplitude * lax.rsqrt(far_re * far_re + far_im * far_im + SMOOTHING)
            resid = jnp.concatenate([(far_re * factor).astype(BF16), (far_im * factor).astype(BF16)], axis=0)
            back = jnp.dot(left_back_ref[...], resid, preferred_element_type=F32).astype(BF16)
            near = jnp.dot(by_lane(back), right_back_ref[...], preferred_element_type=F32)
            for slot, member in enumerate(two):
                wave_re, wave_im = waves[slot]
                cut = slice(slot * side, (slot + 1) * side)
                grad = near[cut, LANES:] * wave_re - near[cut, :LANES] * wave_im
                angle, first, second, offset = place(member)
                turned = pltpu.roll(grad, offset, 1)
                kept = lanes >= offset
                acc[angle, first] += jnp.where(kept, turned, 0.0)
                acc[angle, second] += jnp.where(kept, 0.0, turned)
        return carried

    lax.fori_loop(0, frames // GROUP, step, 0)
    for p in range(pairs):
        for hi in range(2):
            for b in range(own):
                out_ref[p, hi * own + b] = acc[p + hi * pairs, b].astype(WIRE)
        out_ref[p, 2 * own] = halo_join(acc[p, own], acc[p + pairs, own]).astype(WIRE)


def complex_tables(length):
    indices = jnp.arange(length, dtype=jnp.int32)
    product = indices[:, None] * indices[None, :] % length
    phases = product.astype(F32) * (2.0 * math.pi / length)
    cosine, sine = jnp.cos(phases), jnp.sin(phases)
    plus = jnp.block([[cosine, sine], [-sine, cosine]])
    minus = jnp.block([[cosine, -sine], [sine, cosine]])
    scale = 1.0 / length
    return minus.astype(BF16), (plus * scale).astype(BF16), minus.astype(BF16), (plus * scale).astype(BF16)


def frame_gradients(owner, shift, phases, probe, measured, own):
    pairs, pieces, rows, unused = phases.shape
    tables = complex_tables(LANES)
    smem = pl.BlockSpec(memory_space=pltpu.SMEM)
    vmem = pl.BlockSpec(memory_space=pltpu.VMEM)
    return pl.pallas_call(
        functools.partial(frame_kernel, own),
        out_shape=jax.ShapeDtypeStruct(phases.shape, WIRE),
        in_specs=[smem, smem] + [vmem] * 7,
        out_specs=vmem,
        scratch_shapes=[pltpu.VMEM((2 * pairs, own + 1, rows, LANES), F32)],
        compiler_params=pltpu.CompilerParams(vmem_limit_bytes=48 * 1024 * 1024),
        name="frames",
    )(owner, shift, phases, probe, measured, *tables)


def backproject_kernel(slices, blocks, beams, shears_ref, shift_ref, grad_ref, out_ref, near, far, rows_f32, lhs, ker):
    tiles, pairs, pieces = grad_ref.shape[:3]
    angles = 2 * pairs
    own = (pieces - 1) // 2
    half_rows = slices * blocks
    group = pl.program_id(0)
    lanes = lane_ids((slices, LANES))

    @pl.when(group == 0)
    def prepare():
        zero = jnp.zeros((slices, LANES), F32)
        for edge in (0, blocks + 1, blocks + 2):
            near[edge] = zero
            far[edge] = zero
        for a in range(angles):
            hi, p = a // pairs, a % pairs
            margins = []
            for t in range(tiles):
                margin = grad_ref[t, p, 2 * own].astype(F32)
                margins.append(pltpu.roll(margin, HALF, 1) if hi else margin)
            for t in range(tiles):
                for b in range(own):
                    value = grad_ref[t, p, hi * own + b].astype(F32)
                    if b == 0 and t > 0:
                        value += jnp.where(lanes < HALO, margins[t - 1], 0.0)
                    if b == own - 1 and t + 1 < tiles:
                        value += jnp.where(lanes >= LANES - HALO, margins[t + 1], 0.0)
                    k = t * own + b + 1
                    near[k] = pltpu.roll(value, LANES - HALO, 1)
                    far[k] = pltpu.roll(value, LANES - HALO - HALF, 1)
            shift = shift_ref[a, 0]
            for i in range(blocks):
                k = i + 1 + shift
                lower = jnp.where(lanes < LANES - HALO, near[k], near[k + 1])
                upper = jnp.where(lanes < LANES - HALO - HALF, far[k], far[k + 1])
                rows_f32[pl.ds(i, slices, stride=blocks), :] = lower
                rows_f32[pl.ds(half_rows + i, slices, stride=blocks), :] = upper
            lhs[:, a * LANES : (a + 1) * LANES] = rows_f32[...].astype(BF16)

    shape = (LANES, LANES)
    base = (row_ids(shape) - lane_ids(shape) % HALF - HALO).astype(F32) * ROOT
    pick = (lane_ids((1, LANES)) >= HALF).astype(F32)
    for a in range(angles):
        slope = shears_ref[a] * ROOT
        for pair in range(4):
            place = (group * 8 + 2 * pair).astype(F32) - (beams - 1) * 0.5
            gap = base - (pick + place) * slope
            ker[a * LANES : (a + 1) * LANES, pair * LANES : (pair + 1) * LANES] = jnp.exp2(-(gap * gap)).astype(BF16)
    result = jnp.dot(lhs[...], ker[...], preferred_element_type=F32)
    left = lane_ids((half_rows, LANES)) < HALF
    for pair in range(4):
        cols = slice(pair * LANES, (pair + 1) * LANES)
        lower, upper = result[:half_rows, cols], result[half_rows:, cols]
        crossed = pltpu.roll(jnp.where(left, upper, lower), HALF, 1)
        first = jnp.where(left, lower, crossed)
        second = jnp.where(left, crossed, upper)
        for s in range(slices):
            cut = slice(s * blocks, (s + 1) * blocks)
            out_ref[s, 0, pl.ds(2 * pair, blocks, stride=8), :] = first[cut]
            out_ref[s, 0, pl.ds(2 * pair + 1, blocks, stride=8), :] = second[cut]


def backproject(shears, tile_shift, grads, slices, beams, blocks):
    tiles, pairs = grads.shape[:2]
    angles = 2 * pairs
    rows = 2 * slices * blocks
    smem = pl.BlockSpec(memory_space=pltpu.SMEM)
    groups = beams // 8
    result = pl.pallas_call(
        functools.partial(backproject_kernel, slices, blocks, beams),
        out_shape=jax.ShapeDtypeStruct((slices, groups, blocks * 8, LANES), F32),
        grid=(groups,),
        in_specs=[smem, smem, pl.BlockSpec(memory_space=pltpu.VMEM)],
        out_specs=pl.BlockSpec((slices, 1, blocks * 8, LANES), lambda g: (0, g, 0, 0)),
        scratch_shapes=[
            pltpu.VMEM((blocks + 3, slices, LANES), F32),
            pltpu.VMEM((blocks + 3, slices, LANES), F32),
            pltpu.VMEM((rows, LANES), F32),
            pltpu.VMEM((rows, angles * LANES), BF16),
            pltpu.VMEM((angles * LANES, 4 * LANES), BF16),
        ],
        compiler_params=pltpu.CompilerParams(vmem_limit_bytes=48 * 1024 * 1024),
        name="backproject",
    )(shears, tile_shift, grads)
    result = result.reshape(slices, groups, blocks, 8, LANES).transpose(0, 1, 3, 2, 4)
    return result.reshape(slices, beams, blocks * LANES)


def body(volume, shears, tile_shift, illumination, measured, frame_owner, frame_shift):
    tiles, slabs = lax.axis_size("tile"), lax.axis_size("slab")
    slices, beams, width = volume.shape
    blocks = width // LANES
    parts = project(shears, tile_shift, volume, tiles)
    phases = phase_exchange(parts, tiles, slabs)
    grads = frame_gradients(frame_owner, frame_shift, phases, illumination, measured, blocks // tiles)
    gathered = grad_exchange(grads, tiles, slabs)
    return backproject(shears, tile_shift, gathered, slices, beams, blocks)


def solution(mesh):
    in_specs = (
        P("slab", "tile", None),
        P(),
        P(None, "tile"),
        P(),
        P(("slab", "tile"), None, None),
        P(("slab", "tile"), None),
        P(("slab", "tile")),
    )
    out_specs = P("slab", "tile", None)
    return jax.shard_map(body, mesh=mesh, in_specs=in_specs, out_specs=out_specs, check_vma=False)
```

```python
import functools
import math

import jax
import jax.numpy as jnp
import numpy as np
from jax import lax
from jax.experimental import pallas as pl
from jax.experimental.pallas import tpu as pltpu
from jax.sharding import PartitionSpec as P

LANES = 128
HALF = LANES // 2
HALO = 32
SMOOTHING = 0.25
WIRE = jnp.bfloat16
F32 = jnp.float32
BF16 = jnp.bfloat16
MESH = pl.DeviceIdType.MESH
ROOT = math.sqrt(0.5 * math.log2(math.e))
GROUP = 8
SIN_POLY = (3.1415926401307073, -5.1677100835078775, 2.550077523214199, -0.5982912856179897, 0.07765766030124945)
COS_POLY = (0.9999999532476078, -4.934792830619626, 4.0584113528622625, -1.331876568078962, 0.2196896110945085)


def lane_ids(shape):
    return lax.broadcasted_iota(jnp.int32, shape, len(shape) - 1)


def row_ids(shape):
    return lax.broadcasted_iota(jnp.int32, shape, len(shape) - 2)


def halo_join(low, high):
    lanes = lane_ids(low.shape)
    outer = (lanes < HALO) | (lanes >= LANES - HALO)
    return jnp.where(outer, low, pltpu.roll(high, HALF, 1))


def signal_peers(axes):
    barrier = pltpu.get_barrier_semaphore()
    total = 0
    for axis, count in axes:
        me = lax.axis_index(axis)
        for step in range(1, count):
            pl.semaphore_signal(
                barrier, inc=1, device_id={axis: lax.rem(me + step, count)}, device_id_type=MESH
            )
            total += 1
    return barrier, total


def sin_cos(phase):
    turns = phase * (0.5 / math.pi)
    turns = turns - jnp.round(turns)
    square = turns * turns
    sine, cosine = SIN_POLY[-1], COS_POLY[-1]
    for low_s, low_c in zip(SIN_POLY[-2::-1], COS_POLY[-2::-1]):
        sine = sine * square + low_s
        cosine = cosine * square + low_c
    sine = sine * turns
    double = sine + sine
    return double * cosine, 1.0 - double * sine


def phase_kernel(
    tiles, slabs, slices, beams, blocks,
    shears_hbm, shift_hbm, v_hbm, cos_ref, sin_ref,
    shears_ref, shift_ref, v_ref, lhs, ker, res, comb, parts, came, phase,
    small_sem, volume_sem, tile_send, tile_recv, slab_send, slab_recv,
):
    pairs = phase.shape[0]
    own = blocks // tiles
    groups = beams // 8
    half_rows = slices * blocks
    me_t = lax.axis_index("tile")
    me_s = lax.axis_index("slab")
    rows = pl.ds(pl.multiple_of(me_s * slices, slices), slices)

    small = [
        pltpu.make_async_copy(shears_hbm, shears_ref, small_sem.at[0]),
        pltpu.make_async_copy(shift_hbm, shift_ref, small_sem.at[1]),
    ]
    for copy in small:
        copy.start()

    def volume_copy(group):
        return pltpu.make_async_copy(v_hbm.at[:, group], v_ref.at[group], volume_sem.at[group])

    for group in range(groups):
        volume_copy(group).start()
    barrier, greetings = signal_peers((("tile", tiles), ("slab", slabs)))

    def tile_copy(p, step):
        peer = lax.rem(me_t + step, tiles)
        return pltpu.make_async_remote_copy(
            src_ref=parts.at[peer, p],
            dst_ref=came.at[step - 1, p],
            send_sem=tile_send.at[step - 1, p],
            recv_sem=tile_recv.at[step - 1, p],
            device_id={"tile": peer},
            device_id_type=MESH,
        )

    def slab_copy(p, step):
        return pltpu.make_async_remote_copy(
            src_ref=phase.at[p, :, rows, :],
            dst_ref=phase.at[p, :, rows, :],
            send_sem=slab_send.at[step - 1, p],
            recv_sem=slab_recv.at[step - 1, p],
            device_id={"slab": lax.rem(me_s + step, slabs)},
            device_id_type=MESH,
        )

    def arrange(group, carried):
        volume_copy(group).wait()
        for pair in range(4):
            col = pl.multiple_of((group * 4 + pair) * LANES, LANES)
            for duo in range(slices // 2):
                lower, upper = [], []
                for s in (2 * duo, 2 * duo + 1):
                    first = v_ref[group, s, pl.ds(2 * pair, blocks, stride=8), :]
                    second = v_ref[group, s, pl.ds(2 * pair + 1, blocks, stride=8), :]
                    left = lane_ids(first.shape) < HALF
                    crossed = pltpu.roll(jnp.where(left, second, first), HALF, 1)
                    lower.append(jnp.where(left, first, crossed))
                    upper.append(jnp.where(left, crossed, second))
                row = 2 * duo * blocks
                lhs[row : row + 2 * blocks, pl.ds(col, LANES)] = jnp.concatenate(lower, 0).astype(BF16)
                row += half_rows
                lhs[row : row + 2 * blocks, pl.ds(col, LANES)] = jnp.concatenate(upper, 0).astype(BF16)
        return carried

    shape = (HALF, LANES)
    base = (lane_ids(shape) - row_ids(shape) - HALO).astype(F32) * ROOT
    lanes = lane_ids((half_rows, LANES))
    lanes_s = lane_ids((slices, LANES))
    zero = jnp.zeros((slices, LANES), F32)

    def make_beams(p):
        steps = [shears_ref[p] * ROOT, shears_ref[p + pairs] * ROOT]

        def beam(q, carried):
            place = q.astype(F32) - (beams - 1) * 0.5
            row = pl.multiple_of(q * HALF, HALF)
            for side in range(2):
                gap = base - place * steps[side]
                ker[pl.ds(row, HALF), side * LANES : (side + 1) * LANES] = jnp.exp2(-(gap * gap)).astype(BF16)
            return carried

        lax.fori_loop(0, beams, beam, 0, unroll=8)

    def shifted_sums(p, side):
        cols = slice(side * LANES, (side + 1) * LANES)
        near = pltpu.roll(res[0:half_rows, cols], HALO, 1)
        far = pltpu.roll(res[half_rows : 2 * half_rows, cols], HALO + HALF, 1)
        comb[side, 0] = jnp.where(lanes >= HALO, near, 0.0) + jnp.where(lanes >= HALO + HALF, far, 0.0)
        comb[side, 1] = jnp.where(lanes < HALO, near, 0.0) + jnp.where(lanes < HALO + HALF, far, 0.0)
        shift = shift_ref[p + side * pairs]
        row_of = []
        for k in range(blocks):
            total = zero
            for o in range(2):
                i = k - shift - o
                inside = (i >= 0) & (i < blocks)
                picked = comb[side, o, pl.ds(jnp.clip(i, 0, blocks - 1), slices, stride=blocks), :]
                total += jnp.where(inside, picked, 0.0)
            row_of.append(total)
        return row_of

    def project_pair(p):
        res[...] = jnp.dot(lhs[...], ker[...], preferred_element_type=F32)
        sums = [shifted_sums(p, side) for side in range(2)]
        for t in range(tiles):
            margins = []
            for side in range(2):
                for b in range(own):
                    parts[t, p, side * own + b] = sums[side][t * own + b].astype(WIRE)
                after = sums[side][(t + 1) * own] if t + 1 < tiles else zero
                before = sums[side][t * own - 1] if t > 0 else zero
                margins.append(jnp.where(lanes_s < HALF, after, before))
            parts[t, p, 2 * own] = halo_join(margins[0], margins[1]).astype(WIRE)

    for copy in small:
        copy.wait()
    make_beams(0)
    lax.fori_loop(0, groups, arrange, 0)
    project_pair(0)
    pl.semaphore_wait(barrier, greetings)
    for p in range(pairs):
        if p:
            make_beams(p)
            project_pair(p)
        for step in range(1, tiles):
            tile_copy(p, step).start()
    for p in range(pairs):
        total = parts[me_t, p].astype(F32)
        for step in range(1, tiles):
            tile_copy(p, step).wait_recv()
            total += came[step - 1, p].astype(F32)
        phase[p, :, rows, :] = total.astype(WIRE)
        for step in range(1, slabs):
            slab_copy(p, step).start()
    for p in range(pairs):
        for step in range(1, slabs):
            slab_copy(p, step).wait_recv()

        def wave_piece(piece, carried):
            sine, cosine = sin_cos(phase[p, piece].astype(F32))
            sin_ref[p, piece] = sine
            cos_ref[p, piece] = cosine
            return carried

        lax.fori_loop(0, phase.shape[1], wave_piece, 0)
    for p in range(pairs):
        for step in range(1, tiles):
            tile_copy(p, step).wait_send()
        for step in range(1, slabs):
            slab_copy(p, step).wait_send()


def phase_waves(shears, tile_shift, volume, tiles, slabs):
    slices, beams, width = volume.shape
    blocks = width // LANES
    angles = shears.shape[0]
    pairs, own, groups = angles // 2, blocks // tiles, beams // 8
    pieces = 2 * own + 1
    view = volume.reshape(slices, groups, 8, blocks, LANES).transpose(0, 1, 3, 2, 4)
    view = view.reshape(slices, groups, blocks * 8, LANES)
    rows = 2 * slices * blocks
    waves = jax.ShapeDtypeStruct((pairs, pieces, slabs * slices, LANES), F32)
    return pl.pallas_call(
        functools.partial(phase_kernel, tiles, slabs, slices, beams, blocks),
        out_shape=(waves, waves),
        in_specs=[pl.BlockSpec(memory_space=pltpu.HBM)] * 3,
        out_specs=(pl.BlockSpec(memory_space=pltpu.VMEM),) * 2,
        scratch_shapes=[
            pltpu.SMEM((angles,), F32),
            pltpu.SMEM((angles,), jnp.int32),
            pltpu.VMEM((groups, slices, blocks * 8, LANES), F32),
            pltpu.VMEM((rows, beams * HALF), BF16),
            pltpu.VMEM((beams * HALF, 2 * LANES), BF16),
            pltpu.VMEM((rows, 2 * LANES), F32),
            pltpu.VMEM((2, 2, rows // 2, LANES), F32),
            pltpu.VMEM((tiles, pairs, pieces, slices, LANES), WIRE),
            pltpu.VMEM((tiles - 1, pairs, pieces, slices, LANES), WIRE),
            pltpu.VMEM((pairs, pieces, slabs * slices, LANES), WIRE),
            pltpu.SemaphoreType.DMA((2,)),
            pltpu.SemaphoreType.DMA((groups,)),
            pltpu.SemaphoreType.DMA((tiles - 1, pairs)),
            pltpu.SemaphoreType.DMA((tiles - 1, pairs)),
            pltpu.SemaphoreType.DMA((slabs - 1, pairs)),
            pltpu.SemaphoreType.DMA((slabs - 1, pairs)),
        ],
        compiler_params=pltpu.CompilerParams(
            collective_id=0, has_side_effects=True, vmem_limit_bytes=40 * 1024 * 1024
        ),
        name="phase_waves",
    )(
        pltpu.with_memory_space_constraint(shears, pltpu.HBM),
        pltpu.with_memory_space_constraint(tile_shift, pltpu.HBM),
        pltpu.with_memory_space_constraint(view, pltpu.HBM),
    )


def grad_kernel(
    tiles, slabs, blocks, beams,
    shears_ref, shift_ref, grad_ref, lhs_ref, ker_ref,
    gathered, near, far, rows_f32, came, slab_send, slab_recv, tile_send, tile_recv,
):
    pairs, pieces = grad_ref.shape[:2]
    own = (pieces - 1) // 2
    slices = gathered.shape[3]
    half_rows = slices * blocks
    me_t = lax.axis_index("tile")
    me_s = lax.axis_index("slab")
    barrier, greetings = signal_peers((("tile", tiles), ("slab", slabs)))
    pl.semaphore_wait(barrier, greetings)

    def rows_of(slab):
        return pl.ds(pl.multiple_of(slab * slices, slices), slices)

    def slab_copy(p, step):
        peer = lax.rem(me_s + step, slabs)
        return pltpu.make_async_remote_copy(
            src_ref=grad_ref.at[p, :, rows_of(peer), :],
            dst_ref=came.at[step - 1, p],
            send_sem=slab_send.at[step - 1, p],
            recv_sem=slab_recv.at[step - 1, p],
            device_id={"slab": peer},
            device_id_type=MESH,
        )

    def tile_copy(p, step):
        return pltpu.make_async_remote_copy(
            src_ref=gathered.at[me_t, p],
            dst_ref=gathered.at[me_t, p],
            send_sem=tile_send.at[step - 1, p],
            recv_sem=tile_recv.at[step - 1, p],
            device_id={"tile": lax.rem(me_t + step, tiles)},
            device_id_type=MESH,
        )

    for p in range(pairs):
        for step in range(1, slabs):
            slab_copy(p, step).start()

    shape = (LANES, LANES)
    base = (row_ids(shape) - lane_ids(shape) % HALF - HALO).astype(F32) * ROOT
    pick = (lane_ids((1, LANES)) >= HALF).astype(F32) - (beams - 1) * 0.5
    for a in range(2 * pairs):
        slope = shears_ref[a] * ROOT

        def beam(pair, carried):
            gap = base - (pick + (2 * pair).astype(F32)) * slope
            col = pl.multiple_of(pair * LANES, LANES)
            ker_ref[a * LANES : (a + 1) * LANES, pl.ds(col, LANES)] = jnp.exp2(-(gap * gap)).astype(BF16)
            return carried

        lax.fori_loop(0, beams // 2, beam, 0, unroll=8)

    for p in range(pairs):
        total = grad_ref[p, :, rows_of(me_s), :].astype(F32)
        for step in range(1, slabs):
            slab_copy(p, step).wait_recv()
            total += came[step - 1, p].astype(F32)
        gathered[me_t, p] = total.astype(WIRE)
        for step in range(1, tiles):
            tile_copy(p, step).start()

    lanes = lane_ids((slices, LANES))
    zero = jnp.zeros((slices, LANES), F32)
    for edge in (0, blocks + 1, blocks + 2):
        near[edge] = zero
        far[edge] = zero
    for p in range(pairs):
        for step in range(1, tiles):
            tile_copy(p, step).wait_recv()
        for hi in range(2):
            a = p + hi * pairs
            margins = []
            for t in range(tiles):
                margin = gathered[t, p, 2 * own].astype(F32)
                margins.append(pltpu.roll(margin, HALF, 1) if hi else margin)
            for t in range(tiles):
                for b in range(own):
                    value = gathered[t, p, hi * own + b].astype(F32)
                    if b == 0 and t > 0:
                        value += jnp.where(lanes < HALO, margins[t - 1], 0.0)
                    if b == own - 1 and t + 1 < tiles:
                        value += jnp.where(lanes >= LANES - HALO, margins[t + 1], 0.0)
                    k = t * own + b + 1
                    near[k] = pltpu.roll(value, LANES - HALO, 1)
                    far[k] = pltpu.roll(value, LANES - HALO - HALF, 1)
            shift = shift_ref[a]
            for i in range(blocks):
                k = i + 1 + shift
                lower = jnp.where(lanes < LANES - HALO, near[k], near[k + 1])
                upper = jnp.where(lanes < LANES - HALO - HALF, far[k], far[k + 1])
                rows_f32[pl.ds(i, slices, stride=blocks), :] = lower
                rows_f32[pl.ds(half_rows + i, slices, stride=blocks), :] = upper
            lhs_ref[:, a * LANES : (a + 1) * LANES] = rows_f32[...].astype(BF16)
    for p in range(pairs):
        for step in range(1, tiles):
            tile_copy(p, step).wait_send()
        for step in range(1, slabs):
            slab_copy(p, step).wait_send()


def back_operands(shears, tile_shift, grads, tiles, slabs, blocks, beams):
    pairs, pieces, all_rows = grads.shape[:3]
    slices = all_rows // slabs
    angles = 2 * pairs
    rows = 2 * slices * blocks
    smem = pl.BlockSpec(memory_space=pltpu.SMEM)
    vmem = pl.BlockSpec(memory_space=pltpu.VMEM)
    return pl.pallas_call(
        functools.partial(grad_kernel, tiles, slabs, blocks, beams),
        out_shape=(
            jax.ShapeDtypeStruct((rows, angles * LANES), BF16),
            jax.ShapeDtypeStruct((angles * LANES, beams * HALF), BF16),
        ),
        in_specs=[smem, smem, vmem],
        out_specs=(vmem, vmem),
        scratch_shapes=[
            pltpu.VMEM((tiles, pairs, pieces, slices, LANES), WIRE),
            pltpu.VMEM((blocks + 3, slices, LANES), F32),
            pltpu.VMEM((blocks + 3, slices, LANES), F32),
            pltpu.VMEM((rows, LANES), F32),
            pltpu.VMEM((slabs - 1, pairs, pieces, slices, LANES), WIRE),
            pltpu.SemaphoreType.DMA((slabs - 1, pairs)),
            pltpu.SemaphoreType.DMA((slabs - 1, pairs)),
            pltpu.SemaphoreType.DMA((tiles - 1, pairs)),
            pltpu.SemaphoreType.DMA((tiles - 1, pairs)),
        ],
        compiler_params=pltpu.CompilerParams(
            collective_id=1, has_side_effects=True, vmem_limit_bytes=40 * 1024 * 1024
        ),
        name="back_operands",
    )(shears, tile_shift, grads)


def frame_kernel(
    own, owner_ref, start_ref, cos_ref, sin_ref, probe_ref, measured_ref, minus_ref, plus_ref, out_ref, acc,
):
    pairs = cos_ref.shape[0]
    frames, side, unused = measured_ref.shape
    ring = own + 1
    acc[...] = jnp.zeros_like(acc)
    lanes = lane_ids((side, LANES))

    def place(member):
        angle = owner_ref[member]
        start = start_ref[member]
        start = jnp.where(start < 0, start + ring * LANES, start)
        first = start // LANES
        offset = start - first * LANES
        second = jnp.where(first + 1 == ring, 0, first + 1)
        return angle, first, second, offset

    def source(angle, block, offset):
        upper = jnp.where(angle >= pairs, 1, 0)
        margin = block == own
        index = jnp.where(margin, 2 * own, upper * own + block)
        turn = jnp.where(margin, upper * HALF, 0) + LANES - offset
        return angle - upper * pairs, index, jnp.where(turn >= LANES, turn - LANES, turn)

    def by_lane(value):
        return jnp.concatenate(
            [
                jnp.concatenate([value[:side, :LANES], value[side:, :LANES]], axis=1),
                jnp.concatenate([value[:side, LANES:], value[side:, LANES:]], axis=1),
            ],
            axis=0,
        )

    def wave_of(member):
        angle, first, second, offset = place(member)
        pair, index, turn = source(angle, first, offset)
        unused_pair, next_index, next_turn = source(angle, second, offset)
        inner = lanes < LANES - offset

        def window(ref):
            return jnp.where(
                inner, pltpu.roll(ref[pair, index], turn, 1), pltpu.roll(ref[pair, next_index], next_turn, 1)
            )

        cosine, sine = window(cos_ref), window(sin_ref)
        probe_re, probe_im = probe_ref[0], probe_ref[1]
        return probe_re * cosine - probe_im * sine, probe_re * sine + probe_im * cosine

    def add(member, grad):
        angle, first, second, offset = place(member)
        turned = pltpu.roll(grad, offset, 1)
        kept = lanes >= offset
        acc[angle, first] += jnp.where(kept, turned, 0.0)
        acc[angle, second] += jnp.where(kept, 0.0, turned)

    def residual(far, two):
        far_re, far_im = far[:side], far[side:]
        amplitude = jnp.concatenate([measured_ref[member] for member in two], axis=1).astype(F32)
        factor = 1.0 - amplitude * lax.rsqrt(far_re * far_re + far_im * far_im + SMOOTHING)
        return jnp.concatenate([(far_re * factor).astype(BF16), (far_im * factor).astype(BF16)], axis=0)

    def step(number, carried):
        duos = [(number * GROUP + 2 * duo, number * GROUP + 2 * duo + 1) for duo in range(GROUP // 2)]
        waves = [[wave_of(member) for member in two] for two in duos]
        halves = []
        for both in waves:
            stacked = jnp.concatenate(
                [jnp.concatenate([re.astype(BF16), im.astype(BF16)], axis=1) for re, im in both], axis=0
            )
            halves.append(jnp.dot(stacked, minus_ref[...], preferred_element_type=F32).astype(BF16))
        fars = [jnp.dot(plus_ref[...], by_lane(half), preferred_element_type=F32) for half in halves]
        resids = [residual(far, two) for far, two in zip(fars, duos)]
        backs = [jnp.dot(minus_ref[...], resid, preferred_element_type=F32).astype(BF16) for resid in resids]
        nears = [jnp.dot(by_lane(back), plus_ref[...], preferred_element_type=F32) for back in backs]
        for near, two, both in zip(nears, duos, waves):
            for slot, member in enumerate(two):
                wave_re, wave_im = both[slot]
                cut = slice(slot * side, (slot + 1) * side)
                add(member, near[cut, LANES:] * wave_re - near[cut, :LANES] * wave_im)
        return carried

    lax.fori_loop(0, frames // GROUP, step, 0)
    for p in range(pairs):
        for hi in range(2):
            for b in range(own):
                out_ref[p, hi * own + b] = acc[p + hi * pairs, b].astype(WIRE)
        out_ref[p, 2 * own] = halo_join(acc[p, own], acc[p + pairs, own]).astype(WIRE)


def complex_tables(length):
    indices = np.arange(length)
    phases = (indices[:, None] * indices[None, :] % length) * (2.0 * math.pi / length)
    cosine, sine = np.cos(phases), np.sin(phases)
    minus = np.block([[cosine, -sine], [sine, cosine]])
    plus = np.block([[cosine, sine], [-sine, cosine]]) / length
    return jnp.asarray(minus, BF16), jnp.asarray(plus, BF16)


def frame_gradients(owner, shift, cosine, sine, probe, measured, own):
    pairs, pieces, rows, unused = cosine.shape
    smem = pl.BlockSpec(memory_space=pltpu.SMEM)
    vmem = pl.BlockSpec(memory_space=pltpu.VMEM)
    return pl.pallas_call(
        functools.partial(frame_kernel, own),
        out_shape=jax.ShapeDtypeStruct(cosine.shape, WIRE),
        in_specs=[smem, smem] + [vmem] * 6,
        out_specs=vmem,
        scratch_shapes=[pltpu.VMEM((2 * pairs, own + 1, rows, LANES), F32)],
        compiler_params=pltpu.CompilerParams(vmem_limit_bytes=48 * 1024 * 1024),
        name="frames",
    )(owner, shift, cosine, sine, probe, measured, *complex_tables(LANES))


def backproject_kernel(slices, blocks, lhs_ref, ker_ref, out_ref):
    half_rows = slices * blocks
    left = lane_ids((half_rows, LANES)) < HALF
    width = 8 * HALF
    start = pl.multiple_of(pl.program_id(0) * width, width)
    result = jnp.dot(lhs_ref[...], ker_ref[:, pl.ds(start, width)], preferred_element_type=F32)
    for pair in range(4):
        cols = slice(pair * LANES, (pair + 1) * LANES)
        lower, upper = result[:half_rows, cols], result[half_rows:, cols]
        crossed = pltpu.roll(jnp.where(left, upper, lower), HALF, 1)
        first = jnp.where(left, lower, crossed)
        second = jnp.where(left, crossed, upper)
        for s in range(slices):
            cut = slice(s * blocks, (s + 1) * blocks)
            out_ref[s, 0, pl.ds(2 * pair, blocks, stride=8), :] = first[cut]
            out_ref[s, 0, pl.ds(2 * pair + 1, blocks, stride=8), :] = second[cut]


def backproject(lhs, kernels, slices, beams, blocks):
    groups = beams // 8
    result = pl.pallas_call(
        functools.partial(backproject_kernel, slices, blocks),
        out_shape=jax.ShapeDtypeStruct((slices, groups, blocks * 8, LANES), F32),
        grid=(groups,),
        in_specs=[pl.BlockSpec(memory_space=pltpu.VMEM)] * 2,
        out_specs=pl.BlockSpec((slices, 1, blocks * 8, LANES), lambda g: (0, g, 0, 0)),
        compiler_params=pltpu.CompilerParams(vmem_limit_bytes=32 * 1024 * 1024),
        name="backproject",
    )(lhs, kernels)
    result = result.reshape(slices, groups, blocks, 8, LANES).transpose(0, 1, 3, 2, 4)
    return result.reshape(slices, beams, blocks * LANES)


def body(volume, shears, tile_shift, illumination, measured, frame_owner, frame_shift):
    tiles, slabs = lax.axis_size("tile"), lax.axis_size("slab")
    slices, beams, width = volume.shape
    blocks = width // LANES
    offsets = tile_shift.reshape(-1)
    owner = frame_owner.reshape(-1)
    cosine, sine = phase_waves(shears, offsets, volume, tiles, slabs)
    grads = frame_gradients(owner, frame_shift, cosine, sine, illumination, measured, blocks // tiles)
    lhs, kernels = back_operands(shears, offsets, grads, tiles, slabs, blocks, beams)
    return backproject(lhs, kernels, slices, beams, blocks)


def solution(mesh):
    in_specs = (
        P("slab", "tile", None),
        P(),
        P(None, "tile"),
        P(),
        P(("slab", "tile"), None, None),
        P(("slab", "tile"), None),
        P(("slab", "tile")),
    )
    out_specs = P("slab", "tile", None)
    return jax.shard_map(body, mesh=mesh, in_specs=in_specs, out_specs=out_specs, check_vma=False)
```

```python
import functools
import math

import jax
import jax.numpy as jnp
import numpy as np
from jax import lax
from jax.experimental import pallas as pl
from jax.experimental.pallas import tpu as pltpu
from jax.sharding import PartitionSpec as P

LANES = 128
HALF = LANES // 2
HALO = 32
SMOOTHING = 0.25
WIRE = jnp.bfloat16
F32 = jnp.float32
BF16 = jnp.bfloat16
MESH = pl.DeviceIdType.MESH
ROOT = math.sqrt(0.5 * math.log2(math.e))
GROUP = 32
PHASE_CUTS = 4
GRAD_CUTS = 4
SIN_POLY = (3.1415926401307073, -5.1677100835078775, 2.550077523214199, -0.5982912856179897, 0.07765766030124945)
COS_POLY = (0.9999999532476078, -4.934792830619626, 4.0584113528622625, -1.331876568078962, 0.2196896110945085)


def lane_ids(shape):
    return lax.broadcasted_iota(jnp.int32, shape, len(shape) - 1)


def row_ids(shape):
    return lax.broadcasted_iota(jnp.int32, shape, len(shape) - 2)


def halo_join(low, high):
    lanes = lane_ids(low.shape)
    outer = (lanes < HALO) | (lanes >= LANES - HALO)
    return jnp.where(outer, low, pltpu.roll(high, HALF, 1))


def signal_peers(axes):
    barrier = pltpu.get_barrier_semaphore()
    total = 0
    for axis, count in axes:
        me = lax.axis_index(axis)
        for step in range(1, count):
            pl.semaphore_signal(
                barrier, inc=1, device_id={axis: lax.rem(me + step, count)}, device_id_type=MESH
            )
            total += 1
    return barrier, total


def cuts_of(pairs, parts):
    ends = [pairs * part // parts for part in range(parts + 1)]
    return [(low, high) for low, high in zip(ends, ends[1:]) if low < high]


def sin_cos(phase):
    turns = phase * (0.5 / math.pi)
    turns = turns - jnp.round(turns)
    square = turns * turns
    sine, cosine = SIN_POLY[-1], COS_POLY[-1]
    for low_s, low_c in zip(SIN_POLY[-2::-1], COS_POLY[-2::-1]):
        sine = sine * square + low_s
        cosine = cosine * square + low_c
    sine = sine * turns
    double = sine + sine
    return double * cosine, 1.0 - double * sine


def phase_kernel(
    tiles, slabs, slices, beams, blocks,
    shears_hbm, shift_hbm, v_hbm, cos_ref, sin_ref,
    shears_ref, shift_ref, v_ref, lhs, ker, res, comb, parts, came, phase,
    small_sem, volume_sem, tile_send, tile_recv, slab_send, slab_recv,
):
    pairs = phase.shape[0]
    own = blocks // tiles
    groups = beams // 8
    half_rows = slices * blocks
    me_t = lax.axis_index("tile")
    me_s = lax.axis_index("slab")
    rows = pl.ds(pl.multiple_of(me_s * slices, slices), slices)

    small = [
        pltpu.make_async_copy(shears_hbm, shears_ref, small_sem.at[0]),
        pltpu.make_async_copy(shift_hbm, shift_ref, small_sem.at[1]),
    ]
    for copy in small:
        copy.start()

    def volume_copy(group):
        return pltpu.make_async_copy(v_hbm.at[:, group], v_ref.at[group], volume_sem.at[group])

    for group in range(groups):
        volume_copy(group).start()
    barrier, greetings = signal_peers((("tile", tiles), ("slab", slabs)))

    cuts = cuts_of(pairs, PHASE_CUTS)

    def tile_copy(p, step):
        peer = lax.rem(me_t + step, tiles)
        return pltpu.make_async_remote_copy(
            src_ref=parts.at[peer, p],
            dst_ref=came.at[step - 1, p],
            send_sem=tile_send.at[step - 1, p],
            recv_sem=tile_recv.at[step - 1, p],
            device_id={"tile": peer},
            device_id_type=MESH,
        )

    def slab_copy(c, step):
        low, high = cuts[c]
        return pltpu.make_async_remote_copy(
            src_ref=phase.at[low:high, :, rows, :],
            dst_ref=phase.at[low:high, :, rows, :],
            send_sem=slab_send.at[step - 1, c],
            recv_sem=slab_recv.at[step - 1, c],
            device_id={"slab": lax.rem(me_s + step, slabs)},
            device_id_type=MESH,
        )

    shape = (HALF, LANES)
    base = (lane_ids(shape) - row_ids(shape) - HALO).astype(F32) * ROOT
    lanes = lane_ids((half_rows, LANES))
    lanes_s = lane_ids((slices, LANES))
    zero = jnp.zeros((slices, LANES), F32)

    def make_beam_group(p, group):
        steps = [shears_ref[p] * ROOT, shears_ref[p + pairs] * ROOT]
        for beam in range(8):
            q = group * 8 + beam
            place = q.astype(F32) - (beams - 1) * 0.5
            row = pl.multiple_of(q * HALF, HALF)
            for side in range(2):
                gap = base - place * steps[side]
                ker[pl.ds(row, HALF), side * LANES : (side + 1) * LANES] = jnp.exp2(-(gap * gap)).astype(BF16)

    def make_beams(p):
        def group_step(group, carried):
            make_beam_group(p, group)
            return carried

        lax.fori_loop(0, groups, group_step, 0)

    def arrange(group, carried):
        make_beam_group(0, group)
        volume_copy(group).wait()
        for pair in range(4):
            col = pl.multiple_of((group * 4 + pair) * LANES, LANES)
            for duo in range(slices // 2):
                lower, upper = [], []
                for s in (2 * duo, 2 * duo + 1):
                    first = v_ref[group, s, pl.ds(2 * pair, blocks, stride=8), :]
                    second = v_ref[group, s, pl.ds(2 * pair + 1, blocks, stride=8), :]
                    left = lane_ids(first.shape) < HALF
                    crossed = pltpu.roll(jnp.where(left, second, first), HALF, 1)
                    lower.append(jnp.where(left, first, crossed))
                    upper.append(jnp.where(left, crossed, second))
                row = 2 * duo * blocks
                lhs[row : row + 2 * blocks, pl.ds(col, LANES)] = jnp.concatenate(lower, 0).astype(BF16)
                row += half_rows
                lhs[row : row + 2 * blocks, pl.ds(col, LANES)] = jnp.concatenate(upper, 0).astype(BF16)
        return carried

    def shifted_sums(p, side):
        cols = slice(side * LANES, (side + 1) * LANES)
        near = pltpu.roll(res[0:half_rows, cols], HALO, 1)
        far = pltpu.roll(res[half_rows : 2 * half_rows, cols], HALO + HALF, 1)
        comb[side, 0] = jnp.where(lanes >= HALO, near, 0.0) + jnp.where(lanes >= HALO + HALF, far, 0.0)
        comb[side, 1] = jnp.where(lanes < HALO, near, 0.0) + jnp.where(lanes < HALO + HALF, far, 0.0)
        shift = shift_ref[p + side * pairs]
        row_of = []
        for k in range(blocks):
            total = zero
            for o in range(2):
                i = k - shift - o
                inside = (i >= 0) & (i < blocks)
                picked = comb[side, o, pl.ds(jnp.clip(i, 0, blocks - 1), slices, stride=blocks), :]
                total += jnp.where(inside, picked, 0.0)
            row_of.append(total)
        return row_of

    def project_pair(p):
        res[...] = jnp.dot(lhs[...], ker[...], preferred_element_type=F32)
        sums = [shifted_sums(p, side) for side in range(2)]
        for t in range(tiles):
            margins = []
            for side in range(2):
                for b in range(own):
                    parts[t, p, side * own + b] = sums[side][t * own + b].astype(WIRE)
                after = sums[side][(t + 1) * own] if t + 1 < tiles else zero
                before = sums[side][t * own - 1] if t > 0 else zero
                margins.append(jnp.where(lanes_s < HALF, after, before))
            parts[t, p, 2 * own] = halo_join(margins[0], margins[1]).astype(WIRE)

    for copy in small:
        copy.wait()
    lax.fori_loop(0, groups, arrange, 0)
    project_pair(0)
    pl.semaphore_wait(barrier, greetings)
    for p in range(pairs):
        if p:
            make_beams(p)
            project_pair(p)
        for step in range(1, tiles):
            tile_copy(p, step).start()
    for c, (low, high) in enumerate(cuts):
        for p in range(low, high):
            total = parts[me_t, p].astype(F32)
            for step in range(1, tiles):
                tile_copy(p, step).wait_recv()
                total += came[step - 1, p].astype(F32)
            phase[p, :, rows, :] = total.astype(WIRE)
        for step in range(1, slabs):
            slab_copy(c, step).start()
    starts = {low: c for c, (low, high) in enumerate(cuts)}
    for p in range(pairs):
        if p in starts:
            for step in range(1, slabs):
                slab_copy(starts[p], step).wait_recv()

        def wave_piece(piece, carried):
            sine, cosine = sin_cos(phase[p, piece].astype(F32))
            place = piece + jnp.where(piece >= own, 1, 0)
            sin_ref[p, place] = sine
            cos_ref[p, place] = cosine
            return carried

        lax.fori_loop(0, 2 * own, wave_piece, 0)
        sine, cosine = sin_cos(phase[p, 2 * own].astype(F32))
        sin_ref[p, own] = sine
        cos_ref[p, own] = cosine
        sin_ref[p, 2 * own + 1] = pltpu.roll(sine, HALF, 1)
        cos_ref[p, 2 * own + 1] = pltpu.roll(cosine, HALF, 1)
    for p in range(pairs):
        for step in range(1, tiles):
            tile_copy(p, step).wait_send()
    for c in range(len(cuts)):
        for step in range(1, slabs):
            slab_copy(c, step).wait_send()


def phase_waves(shears, tile_shift, volume, tiles, slabs):
    slices, beams, width = volume.shape
    blocks = width // LANES
    angles = shears.shape[0]
    pairs, own, groups = angles // 2, blocks // tiles, beams // 8
    pieces = 2 * own + 1
    view = volume.reshape(slices, groups, 8, blocks, LANES).transpose(0, 1, 3, 2, 4)
    view = view.reshape(slices, groups, blocks * 8, LANES)
    rows = 2 * slices * blocks
    waves = jax.ShapeDtypeStruct((pairs, 2 * (own + 1), slabs * slices, LANES), F32)
    return pl.pallas_call(
        functools.partial(phase_kernel, tiles, slabs, slices, beams, blocks),
        out_shape=(waves, waves),
        in_specs=[pl.BlockSpec(memory_space=pltpu.HBM)] * 3,
        out_specs=(pl.BlockSpec(memory_space=pltpu.VMEM),) * 2,
        scratch_shapes=[
            pltpu.SMEM((angles,), F32),
            pltpu.SMEM((angles,), jnp.int32),
            pltpu.VMEM((groups, slices, blocks * 8, LANES), F32),
            pltpu.VMEM((rows, beams * HALF), BF16),
            pltpu.VMEM((beams * HALF, 2 * LANES), BF16),
            pltpu.VMEM((rows, 2 * LANES), F32),
            pltpu.VMEM((2, 2, rows // 2, LANES), F32),
            pltpu.VMEM((tiles, pairs, pieces, slices, LANES), WIRE),
            pltpu.VMEM((tiles - 1, pairs, pieces, slices, LANES), WIRE),
            pltpu.VMEM((pairs, pieces, slabs * slices, LANES), WIRE),
            pltpu.SemaphoreType.DMA((2,)),
            pltpu.SemaphoreType.DMA((groups,)),
            pltpu.SemaphoreType.DMA((tiles - 1, pairs)),
            pltpu.SemaphoreType.DMA((tiles - 1, pairs)),
            pltpu.SemaphoreType.DMA((slabs - 1, pairs)),
            pltpu.SemaphoreType.DMA((slabs - 1, pairs)),
        ],
        compiler_params=pltpu.CompilerParams(
            collective_id=0, has_side_effects=True, vmem_limit_bytes=40 * 1024 * 1024
        ),
        name="phase_waves",
    )(
        pltpu.with_memory_space_constraint(shears, pltpu.HBM),
        pltpu.with_memory_space_constraint(tile_shift, pltpu.HBM),
        pltpu.with_memory_space_constraint(view, pltpu.HBM),
    )


def grad_kernel(
    tiles, slabs, blocks, beams,
    shears_ref, shift_ref, grad_ref, lhs_ref, ker_ref,
    gathered, near, far, rows_f32, came, slab_send, slab_recv, tile_send, tile_recv,
):
    pairs, pieces = grad_ref.shape[:2]
    own = (pieces - 1) // 2
    slices = gathered.shape[3]
    half_rows = slices * blocks
    me_t = lax.axis_index("tile")
    me_s = lax.axis_index("slab")
    barrier, greetings = signal_peers((("tile", tiles), ("slab", slabs)))

    def rows_of(slab):
        return pl.ds(pl.multiple_of(slab * slices, slices), slices)

    cuts = cuts_of(pairs, GRAD_CUTS)

    def slab_copy(c, step):
        peer = lax.rem(me_s + step, slabs)
        low, high = cuts[c]
        return pltpu.make_async_remote_copy(
            src_ref=grad_ref.at[low:high, :, rows_of(peer), :],
            dst_ref=came.at[step - 1, low:high],
            send_sem=slab_send.at[step - 1, c],
            recv_sem=slab_recv.at[step - 1, c],
            device_id={"slab": peer},
            device_id_type=MESH,
        )

    def tile_copy(c, step):
        low, high = cuts[c]
        return pltpu.make_async_remote_copy(
            src_ref=gathered.at[me_t, low:high],
            dst_ref=gathered.at[me_t, low:high],
            send_sem=tile_send.at[step - 1, c],
            recv_sem=tile_recv.at[step - 1, c],
            device_id={"tile": lax.rem(me_t + step, tiles)},
            device_id_type=MESH,
        )

    shape = (LANES, LANES)
    base = (row_ids(shape) - lane_ids(shape) % HALF - HALO).astype(F32) * ROOT
    pick = (lane_ids((1, LANES)) >= HALF).astype(F32) - (beams - 1) * 0.5

    def make_beams(angles):
        for a in angles:
            slope = shears_ref[a] * ROOT

            def beam(pair, carried):
                gap = base - (pick + (2 * pair).astype(F32)) * slope
                col = pl.multiple_of(pair * LANES, LANES)
                ker_ref[a * LANES : (a + 1) * LANES, pl.ds(col, LANES)] = jnp.exp2(-(gap * gap)).astype(BF16)
                return carried

            lax.fori_loop(0, beams // 2, beam, 0, unroll=8)

    early = pairs // 2
    make_beams(range(early))
    pl.semaphore_wait(barrier, greetings)
    for c in range(len(cuts)):
        for step in range(1, slabs):
            slab_copy(c, step).start()
    make_beams(range(early, 2 * pairs))

    for c, (low, high) in enumerate(cuts):
        for step in range(1, slabs):
            slab_copy(c, step).wait_recv()
        for p in range(low, high):
            total = grad_ref[p, :, rows_of(me_s), :].astype(F32)
            for step in range(1, slabs):
                total += came[step - 1, p].astype(F32)
            gathered[me_t, p] = total.astype(WIRE)
        for step in range(1, tiles):
            tile_copy(c, step).start()

    lanes = lane_ids((slices, LANES))
    zero = jnp.zeros((slices, LANES), F32)
    for edge in (0, blocks + 1, blocks + 2):
        near[edge] = zero
        far[edge] = zero
    starts = {low: c for c, (low, high) in enumerate(cuts)}
    for p in range(pairs):
        if p in starts:
            for step in range(1, tiles):
                tile_copy(starts[p], step).wait_recv()
        for hi in range(2):
            a = p + hi * pairs
            margins = []
            for t in range(tiles):
                margin = gathered[t, p, 2 * own].astype(F32)
                margins.append(pltpu.roll(margin, HALF, 1) if hi else margin)
            for t in range(tiles):
                for b in range(own):
                    value = gathered[t, p, hi * own + b].astype(F32)
                    if b == 0 and t > 0:
                        value += jnp.where(lanes < HALO, margins[t - 1], 0.0)
                    if b == own - 1 and t + 1 < tiles:
                        value += jnp.where(lanes >= LANES - HALO, margins[t + 1], 0.0)
                    k = t * own + b + 1
                    near[k] = pltpu.roll(value, LANES - HALO, 1)
                    far[k] = pltpu.roll(value, LANES - HALO - HALF, 1)
            shift = shift_ref[a]
            for i in range(blocks):
                k = i + 1 + shift
                lower = jnp.where(lanes < LANES - HALO, near[k], near[k + 1])
                upper = jnp.where(lanes < LANES - HALO - HALF, far[k], far[k + 1])
                rows_f32[pl.ds(i, slices, stride=blocks), :] = lower
                rows_f32[pl.ds(half_rows + i, slices, stride=blocks), :] = upper
            lhs_ref[:, a * LANES : (a + 1) * LANES] = rows_f32[...].astype(BF16)
    for c in range(len(cuts)):
        for step in range(1, tiles):
            tile_copy(c, step).wait_send()
        for step in range(1, slabs):
            slab_copy(c, step).wait_send()


def back_operands(shears, tile_shift, grads, tiles, slabs, blocks, beams):
    pairs, pieces, all_rows = grads.shape[:3]
    slices = all_rows // slabs
    angles = 2 * pairs
    rows = 2 * slices * blocks
    smem = pl.BlockSpec(memory_space=pltpu.SMEM)
    vmem = pl.BlockSpec(memory_space=pltpu.VMEM)
    return pl.pallas_call(
        functools.partial(grad_kernel, tiles, slabs, blocks, beams),
        out_shape=(
            jax.ShapeDtypeStruct((rows, angles * LANES), BF16),
            jax.ShapeDtypeStruct((angles * LANES, beams * HALF), BF16),
        ),
        in_specs=[smem, smem, vmem],
        out_specs=(vmem, vmem),
        scratch_shapes=[
            pltpu.VMEM((tiles, pairs, pieces, slices, LANES), WIRE),
            pltpu.VMEM((blocks + 3, slices, LANES), F32),
            pltpu.VMEM((blocks + 3, slices, LANES), F32),
            pltpu.VMEM((rows, LANES), F32),
            pltpu.VMEM((slabs - 1, pairs, pieces, slices, LANES), WIRE),
            pltpu.SemaphoreType.DMA((slabs - 1, pairs)),
            pltpu.SemaphoreType.DMA((slabs - 1, pairs)),
            pltpu.SemaphoreType.DMA((tiles - 1, pairs)),
            pltpu.SemaphoreType.DMA((tiles - 1, pairs)),
        ],
        compiler_params=pltpu.CompilerParams(
            collective_id=1, has_side_effects=True, vmem_limit_bytes=40 * 1024 * 1024
        ),
        name="back_operands",
    )(shears, tile_shift, grads)


def frame_kernel(
    own, owner_ref, start_ref, cos_ref, sin_ref, probe_ref, measured_ref, minus_ref, plus_ref, out_ref, acc,
):
    pairs = cos_ref.shape[0]
    frames, side, unused = measured_ref.shape
    ring = own + 1
    acc[...] = jnp.zeros_like(acc)
    lanes = lane_ids((side, LANES))

    def place(member):
        angle = owner_ref[member]
        start = start_ref[member]
        start = jnp.where(start < 0, start + ring * LANES, start)
        first = start // LANES
        offset = start - first * LANES
        second = jnp.where(first + 1 == ring, 0, first + 1)
        return angle, first, second, offset

    def by_lane(value):
        return jnp.concatenate(
            [
                jnp.concatenate([value[:side, :LANES], value[side:, :LANES]], axis=1),
                jnp.concatenate([value[:side, LANES:], value[side:, LANES:]], axis=1),
            ],
            axis=0,
        )

    def wave_of(member):
        angle, first, second, offset = place(member)
        upper = jnp.where(angle >= pairs, 1, 0)
        pair = angle - upper * pairs
        outer = lanes >= offset
        turn = jnp.where(offset > 0, LANES - offset, 0)

        def window(ref):
            return pltpu.roll(jnp.where(outer, ref[pair, upper * ring + first], ref[pair, upper * ring + second]), turn, 1)

        cosine, sine = window(cos_ref), window(sin_ref)
        probe_re, probe_im = probe_ref[0], probe_ref[1]
        return probe_re * cosine - probe_im * sine, probe_re * sine + probe_im * cosine

    def add(member, grad):
        angle, first, second, offset = place(member)
        turned = pltpu.roll(grad, offset, 1)
        kept = lanes >= offset
        acc[angle, first] += jnp.where(kept, turned, 0.0)
        acc[angle, second] += jnp.where(kept, 0.0, turned)

    def residual(far, two):
        far_re, far_im = far[:side], far[side:]
        amplitude = jnp.concatenate([measured_ref[member] for member in two], axis=1).astype(F32)
        factor = 1.0 - amplitude * lax.rsqrt(far_re * far_re + far_im * far_im + SMOOTHING)
        return jnp.concatenate([(far_re * factor).astype(BF16), (far_im * factor).astype(BF16)], axis=0)

    def step(number, carried):
        duos = [(number * GROUP + 2 * duo, number * GROUP + 2 * duo + 1) for duo in range(GROUP // 2)]
        waves = [[wave_of(member) for member in two] for two in duos]
        halves = []
        for both in waves:
            stacked = jnp.concatenate(
                [jnp.concatenate([re.astype(BF16), im.astype(BF16)], axis=1) for re, im in both], axis=0
            )
            halves.append(jnp.dot(stacked, minus_ref[...], preferred_element_type=F32).astype(BF16))
        fars = [jnp.dot(plus_ref[...], by_lane(half), preferred_element_type=F32) for half in halves]
        resids = [residual(far, two) for far, two in zip(fars, duos)]
        backs = [jnp.dot(minus_ref[...], resid, preferred_element_type=F32).astype(BF16) for resid in resids]
        nears = [jnp.dot(by_lane(back), plus_ref[...], preferred_element_type=F32) for back in backs]
        for near, two, both in zip(nears, duos, waves):
            for slot, member in enumerate(two):
                wave_re, wave_im = both[slot]
                cut = slice(slot * side, (slot + 1) * side)
                add(member, near[cut, LANES:] * wave_re - near[cut, :LANES] * wave_im)
        return carried

    lax.fori_loop(0, frames // GROUP, step, 0)
    for p in range(pairs):
        for hi in range(2):
            for b in range(own):
                out_ref[p, hi * own + b] = acc[p + hi * pairs, b].astype(WIRE)
        out_ref[p, 2 * own] = halo_join(acc[p, own], acc[p + pairs, own]).astype(WIRE)


def complex_tables(length):
    indices = np.arange(length)
    phases = (indices[:, None] * indices[None, :] % length) * (2.0 * math.pi / length)
    cosine, sine = np.cos(phases), np.sin(phases)
    minus = np.block([[cosine, -sine], [sine, cosine]])
    plus = np.block([[cosine, sine], [-sine, cosine]]) / length
    return jnp.asarray(minus, BF16), jnp.asarray(plus, BF16)


def frame_gradients(owner, shift, cosine, sine, probe, measured, own):
    pairs, waves, rows, unused = cosine.shape
    smem = pl.BlockSpec(memory_space=pltpu.SMEM)
    vmem = pl.BlockSpec(memory_space=pltpu.VMEM)
    return pl.pallas_call(
        functools.partial(frame_kernel, own),
        out_shape=jax.ShapeDtypeStruct((pairs, waves - 1, rows, LANES), WIRE),
        in_specs=[smem, smem] + [vmem] * 6,
        out_specs=vmem,
        scratch_shapes=[pltpu.VMEM((2 * pairs, own + 1, rows, LANES), F32)],
        compiler_params=pltpu.CompilerParams(vmem_limit_bytes=48 * 1024 * 1024),
        name="frames",
    )(owner, shift, cosine, sine, probe, measured, *complex_tables(LANES))


def backproject_kernel(slices, blocks, beams, lhs_ref, ker_ref, out_hbm, out_ref, sems):
    groups = beams // 8
    width = 8 * HALF
    half_rows = slices * blocks
    left = lane_ids((half_rows, LANES)) < HALF

    def copy_out(group):
        return pltpu.make_async_copy(out_ref.at[:, group], out_hbm.at[:, group], sems.at[group])

    def step(group, carried):
        start = pl.multiple_of(group * width, width)
        result = jnp.dot(lhs_ref[...], ker_ref[:, pl.ds(start, width)], preferred_element_type=F32)
        for pair in range(4):
            cols = slice(pair * LANES, (pair + 1) * LANES)
            lower, upper = result[:half_rows, cols], result[half_rows:, cols]
            crossed = pltpu.roll(jnp.where(left, upper, lower), HALF, 1)
            first = jnp.where(left, lower, crossed)
            second = jnp.where(left, crossed, upper)
            for s in range(slices):
                cut = slice(s * blocks, (s + 1) * blocks)
                out_ref[s, group, pl.ds(2 * pair, blocks, stride=8), :] = first[cut]
                out_ref[s, group, pl.ds(2 * pair + 1, blocks, stride=8), :] = second[cut]
        copy_out(group).start()
        return carried

    lax.fori_loop(0, groups, step, 0, unroll=True)

    def finish(group, carried):
        copy_out(group).wait()
        return carried

    lax.fori_loop(0, groups, finish, 0)


def backproject(lhs, kernels, slices, beams, blocks):
    groups = beams // 8
    shape = (slices, groups, blocks * 8, LANES)
    result = pl.pallas_call(
        functools.partial(backproject_kernel, slices, blocks, beams),
        out_shape=jax.ShapeDtypeStruct(shape, F32),
        in_specs=[pl.BlockSpec(memory_space=pltpu.VMEM)] * 2,
        out_specs=pl.BlockSpec(memory_space=pltpu.HBM),
        scratch_shapes=[pltpu.VMEM(shape, F32), pltpu.SemaphoreType.DMA((groups,))],
        compiler_params=pltpu.CompilerParams(vmem_limit_bytes=32 * 1024 * 1024),
        name="backproject",
    )(lhs, kernels)
    result = result.reshape(slices, groups, blocks, 8, LANES).transpose(0, 1, 3, 2, 4)
    return result.reshape(slices, beams, blocks * LANES)


def body(volume, shears, tile_shift, illumination, measured, frame_owner, frame_shift):
    tiles, slabs = lax.axis_size("tile"), lax.axis_size("slab")
    slices, beams, width = volume.shape
    blocks = width // LANES
    offsets = tile_shift.reshape(-1)
    owner = frame_owner.reshape(-1)
    cosine, sine = phase_waves(shears, offsets, volume, tiles, slabs)
    grads = frame_gradients(owner, frame_shift, cosine, sine, illumination, measured, blocks // tiles)
    lhs, kernels = back_operands(shears, offsets, grads, tiles, slabs, blocks, beams)
    return backproject(lhs, kernels, slices, beams, blocks)


def solution(mesh):
    in_specs = (
        P("slab", "tile", None),
        P(),
        P(None, "tile"),
        P(),
        P(("slab", "tile"), None, None),
        P(("slab", "tile"), None),
        P(("slab", "tile")),
    )
    out_specs = P("slab", "tile", None)
    return jax.shard_map(body, mesh=mesh, in_specs=in_specs, out_specs=out_specs, check_vma=False)
```

```python
import functools
import math

import jax
import jax.numpy as jnp
import numpy as np
from jax import lax
from jax.experimental import pallas as pl
from jax.experimental.pallas import tpu as pltpu
from jax.sharding import PartitionSpec as P

LANES = 128
HALF = LANES // 2
HALO = 32
SMOOTHING = 0.25
WIRE = jnp.bfloat16
F32 = jnp.float32
BF16 = jnp.bfloat16
MESH = pl.DeviceIdType.MESH
ROOT = math.sqrt(0.5 * math.log2(math.e))
GROUP = 32
PHASE_CUTS = 4
GRAD_CUTS = 4
SIN_POLY = (3.1415926401307073, -5.1677100835078775, 2.550077523214199, -0.5982912856179897, 0.07765766030124945)
COS_POLY = (0.9999999532476078, -4.934792830619626, 4.0584113528622625, -1.331876568078962, 0.2196896110945085)


def lane_ids(shape):
    return lax.broadcasted_iota(jnp.int32, shape, len(shape) - 1)


def row_ids(shape):
    return lax.broadcasted_iota(jnp.int32, shape, len(shape) - 2)


def halo_join(low, high):
    lanes = lane_ids(low.shape)
    outer = (lanes < HALO) | (lanes >= LANES - HALO)
    return jnp.where(outer, low, pltpu.roll(high, HALF, 1))


def signal_peers(axes):
    barrier = pltpu.get_barrier_semaphore()
    total = 0
    for axis, count in axes:
        me = lax.axis_index(axis)
        for step in range(1, count):
            pl.semaphore_signal(
                barrier, inc=1, device_id={axis: lax.rem(me + step, count)}, device_id_type=MESH
            )
            total += 1
    return barrier, total


def cuts_of(pairs, parts):
    ends = [pairs * part // parts for part in range(parts + 1)]
    return [(low, high) for low, high in zip(ends, ends[1:]) if low < high]


def sin_cos(phase):
    turns = phase * (0.5 / math.pi)
    turns = turns - jnp.round(turns)
    square = turns * turns
    sine, cosine = SIN_POLY[-1], COS_POLY[-1]
    for low_s, low_c in zip(SIN_POLY[-2::-1], COS_POLY[-2::-1]):
        sine = sine * square + low_s
        cosine = cosine * square + low_c
    sine = sine * turns
    double = sine + sine
    return double * cosine, 1.0 - double * sine


def phase_kernel(
    tiles, slabs, slices, beams, blocks,
    shears_hbm, shift_hbm, v_hbm, cos_ref, sin_ref,
    shears_ref, shift_ref, v_ref, lhs, ker, res, comb, parts, came, phase,
    small_sem, volume_sem, tile_send, tile_recv, slab_send, slab_recv,
):
    pairs = phase.shape[0]
    own = blocks // tiles
    groups = beams // 8
    half_rows = slices * blocks
    me_t = lax.axis_index("tile")
    me_s = lax.axis_index("slab")
    rows = pl.ds(pl.multiple_of(me_s * slices, slices), slices)

    small = [
        pltpu.make_async_copy(shears_hbm, shears_ref, small_sem.at[0]),
        pltpu.make_async_copy(shift_hbm, shift_ref, small_sem.at[1]),
    ]
    for copy in small:
        copy.start()

    def volume_copy(group):
        return pltpu.make_async_copy(v_hbm.at[:, group], v_ref.at[group], volume_sem.at[group])

    for group in range(groups):
        volume_copy(group).start()
    barrier, greetings = signal_peers((("tile", tiles), ("slab", slabs)))

    cuts = cuts_of(pairs, PHASE_CUTS)

    def tile_copy(p, step):
        peer = lax.rem(me_t + step, tiles)
        return pltpu.make_async_remote_copy(
            src_ref=parts.at[peer, p],
            dst_ref=came.at[step - 1, p],
            send_sem=tile_send.at[step - 1, p],
            recv_sem=tile_recv.at[step - 1, p],
            device_id={"tile": peer},
            device_id_type=MESH,
        )

    def slab_copy(c, step):
        low, high = cuts[c]
        return pltpu.make_async_remote_copy(
            src_ref=phase.at[low:high, :, rows, :],
            dst_ref=phase.at[low:high, :, rows, :],
            send_sem=slab_send.at[step - 1, c],
            recv_sem=slab_recv.at[step - 1, c],
            device_id={"slab": lax.rem(me_s + step, slabs)},
            device_id_type=MESH,
        )

    shape = (16, LANES)
    base = (lane_ids(shape) - row_ids(shape) - HALO).astype(F32) * ROOT
    lanes = lane_ids((half_rows, LANES))
    lanes_s = lane_ids((slices, LANES))
    zero = jnp.zeros((slices, LANES), F32)

    def make_beam_group(p, group):
        steps = [shears_ref[p] * ROOT, shears_ref[p + pairs] * ROOT]
        for beam in range(8):
            q = group * 8 + beam
            place = jnp.asarray(q, F32) - (beams - 1) * 0.5
            row = q * HALF if isinstance(q, int) else pl.multiple_of(q * HALF, HALF)
            for side in range(2):
                gap = base - place * steps[side]
                rows_of = jnp.exp2(-(gap * gap)).astype(BF16)
                for turn in range(HALF // 16):
                    turned = pltpu.roll(rows_of, 16 * turn, 1) if turn else rows_of
                    ker[p % 2, pl.ds(row + 16 * turn, 16), side * LANES : (side + 1) * LANES] = turned

    def make_beams(p):
        for group in range(groups):
            make_beam_group(p, group)

    def arrange(group, carried):
        volume_copy(group).wait()
        for pair in range(4):
            col = pl.multiple_of((group * 4 + pair) * LANES, LANES)
            for duo in range(slices // 2):
                lower, upper = [], []
                for s in (2 * duo, 2 * duo + 1):
                    first = v_ref[group, s, pl.ds(2 * pair, blocks, stride=8), :]
                    second = v_ref[group, s, pl.ds(2 * pair + 1, blocks, stride=8), :]
                    left = lane_ids(first.shape) < HALF
                    crossed = pltpu.roll(jnp.where(left, second, first), HALF, 1)
                    lower.append(jnp.where(left, first, crossed))
                    upper.append(jnp.where(left, crossed, second))
                row = 2 * duo * blocks
                lhs[row : row + 2 * blocks, pl.ds(col, LANES)] = jnp.concatenate(lower, 0).astype(BF16)
                row += half_rows
                lhs[row : row + 2 * blocks, pl.ds(col, LANES)] = jnp.concatenate(upper, 0).astype(BF16)
        return carried

    def shifted_sums(p, side):
        cols = slice(side * LANES, (side + 1) * LANES)
        near = pltpu.roll(res[0:half_rows, cols], HALO, 1)
        far = pltpu.roll(res[half_rows : 2 * half_rows, cols], HALO + HALF, 1)
        comb[side, 0] = jnp.where(lanes >= HALO, near, 0.0) + jnp.where(lanes >= HALO + HALF, far, 0.0)
        comb[side, 1] = jnp.where(lanes < HALO, near, 0.0) + jnp.where(lanes < HALO + HALF, far, 0.0)
        shift = shift_ref[p + side * pairs]
        row_of = []
        for k in range(blocks):
            total = zero
            for o in range(2):
                i = k - shift - o
                inside = (i >= 0) & (i < blocks)
                picked = comb[side, o, pl.ds(jnp.clip(i, 0, blocks - 1), slices, stride=blocks), :]
                total += jnp.where(inside, picked, 0.0)
            row_of.append(total)
        return row_of

    def project_pair(p):
        if p:
            make_beams(p)
        res[...] = jnp.dot(lhs[...], ker[p % 2], preferred_element_type=F32)
        sums = [shifted_sums(p, side) for side in range(2)]
        for t in range(tiles):
            margins = []
            for side in range(2):
                for b in range(own):
                    parts[t, p, side * own + b] = sums[side][t * own + b].astype(WIRE)
                after = sums[side][(t + 1) * own] if t + 1 < tiles else zero
                before = sums[side][t * own - 1] if t > 0 else zero
                margins.append(jnp.where(lanes_s < HALF, after, before))
            parts[t, p, 2 * own] = halo_join(margins[0], margins[1]).astype(WIRE)

    for copy in small:
        copy.wait()
    make_beams(0)
    lax.fori_loop(0, groups, arrange, 0)
    project_pair(0)
    pl.semaphore_wait(barrier, greetings)
    for p in range(pairs):
        if p:
            project_pair(p)
        for step in range(1, tiles):
            tile_copy(p, step).start()
    for c, (low, high) in enumerate(cuts):
        for p in range(low, high):
            total = parts[me_t, p].astype(F32)
            for step in range(1, tiles):
                tile_copy(p, step).wait_recv()
                total += came[step - 1, p].astype(F32)
            phase[p, :, rows, :] = total.astype(WIRE)
        for step in range(1, slabs):
            slab_copy(c, step).start()
    starts = {low: c for c, (low, high) in enumerate(cuts)}
    for p in range(pairs):
        if p in starts:
            for step in range(1, slabs):
                slab_copy(starts[p], step).wait_recv()

        def wave_piece(piece, carried):
            sine, cosine = sin_cos(phase[p, piece].astype(F32))
            place = piece + jnp.where(piece >= own, 1, 0)
            sin_ref[p, place] = sine
            cos_ref[p, place] = cosine
            return carried

        lax.fori_loop(0, 2 * own, wave_piece, 0)
        sine, cosine = sin_cos(phase[p, 2 * own].astype(F32))
        sin_ref[p, own] = sine
        cos_ref[p, own] = cosine
        sin_ref[p, 2 * own + 1] = pltpu.roll(sine, HALF, 1)
        cos_ref[p, 2 * own + 1] = pltpu.roll(cosine, HALF, 1)
    for p in range(pairs):
        for step in range(1, tiles):
            tile_copy(p, step).wait_send()
    for c in range(len(cuts)):
        for step in range(1, slabs):
            slab_copy(c, step).wait_send()


def phase_waves(shears, tile_shift, volume, tiles, slabs):
    slices, beams, width = volume.shape
    blocks = width // LANES
    angles = shears.shape[0]
    pairs, own, groups = angles // 2, blocks // tiles, beams // 8
    pieces = 2 * own + 1
    view = volume.reshape(slices, groups, 8, blocks, LANES).transpose(0, 1, 3, 2, 4)
    view = view.reshape(slices, groups, blocks * 8, LANES)
    rows = 2 * slices * blocks
    waves = jax.ShapeDtypeStruct((pairs, 2 * (own + 1), slabs * slices, LANES), F32)
    return pl.pallas_call(
        functools.partial(phase_kernel, tiles, slabs, slices, beams, blocks),
        out_shape=(waves, waves),
        in_specs=[pl.BlockSpec(memory_space=pltpu.HBM)] * 3,
        out_specs=(pl.BlockSpec(memory_space=pltpu.VMEM),) * 2,
        scratch_shapes=[
            pltpu.SMEM((angles,), F32),
            pltpu.SMEM((angles,), jnp.int32),
            pltpu.VMEM((groups, slices, blocks * 8, LANES), F32),
            pltpu.VMEM((rows, beams * HALF), BF16),
            pltpu.VMEM((2, beams * HALF, 2 * LANES), BF16),
            pltpu.VMEM((rows, 2 * LANES), F32),
            pltpu.VMEM((2, 2, rows // 2, LANES), F32),
            pltpu.VMEM((tiles, pairs, pieces, slices, LANES), WIRE),
            pltpu.VMEM((tiles - 1, pairs, pieces, slices, LANES), WIRE),
            pltpu.VMEM((pairs, pieces, slabs * slices, LANES), WIRE),
            pltpu.SemaphoreType.DMA((2,)),
            pltpu.SemaphoreType.DMA((groups,)),
            pltpu.SemaphoreType.DMA((tiles - 1, pairs)),
            pltpu.SemaphoreType.DMA((tiles - 1, pairs)),
            pltpu.SemaphoreType.DMA((slabs - 1, pairs)),
            pltpu.SemaphoreType.DMA((slabs - 1, pairs)),
        ],
        compiler_params=pltpu.CompilerParams(
            collective_id=0, has_side_effects=True, vmem_limit_bytes=40 * 1024 * 1024
        ),
        name="phase_waves",
    )(
        pltpu.with_memory_space_constraint(shears, pltpu.HBM),
        pltpu.with_memory_space_constraint(tile_shift, pltpu.HBM),
        pltpu.with_memory_space_constraint(view, pltpu.HBM),
    )


def grad_kernel(
    tiles, slabs, blocks, beams,
    shears_ref, shift_ref, grad_ref, lhs_ref, ker_ref,
    gathered, near, far, rows_f32, came, slab_send, slab_recv, tile_send, tile_recv,
):
    pairs, pieces = grad_ref.shape[:2]
    own = (pieces - 1) // 2
    slices = gathered.shape[3]
    half_rows = slices * blocks
    me_t = lax.axis_index("tile")
    me_s = lax.axis_index("slab")
    barrier, greetings = signal_peers((("tile", tiles), ("slab", slabs)))

    def rows_of(slab):
        return pl.ds(pl.multiple_of(slab * slices, slices), slices)

    cuts = cuts_of(pairs, GRAD_CUTS)

    def slab_copy(c, step):
        peer = lax.rem(me_s + step, slabs)
        low, high = cuts[c]
        return pltpu.make_async_remote_copy(
            src_ref=grad_ref.at[low:high, :, rows_of(peer), :],
            dst_ref=came.at[step - 1, low:high],
            send_sem=slab_send.at[step - 1, c],
            recv_sem=slab_recv.at[step - 1, c],
            device_id={"slab": peer},
            device_id_type=MESH,
        )

    def tile_copy(c, step):
        low, high = cuts[c]
        return pltpu.make_async_remote_copy(
            src_ref=gathered.at[me_t, low:high],
            dst_ref=gathered.at[me_t, low:high],
            send_sem=tile_send.at[step - 1, c],
            recv_sem=tile_recv.at[step - 1, c],
            device_id={"tile": lax.rem(me_t + step, tiles)},
            device_id_type=MESH,
        )

    shape = (LANES, LANES)
    base = (row_ids(shape) - lane_ids(shape) % HALF - HALO).astype(F32) * ROOT
    pick = (lane_ids((1, LANES)) >= HALF).astype(F32) - (beams - 1) * 0.5

    def make_beams(angles):
        for a in angles:
            slope = shears_ref[a] * ROOT

            def beam(pair, carried):
                gap = base - (pick + (2 * pair).astype(F32)) * slope
                col = pl.multiple_of(pair * LANES, LANES)
                ker_ref[a * LANES : (a + 1) * LANES, pl.ds(col, LANES)] = jnp.exp2(-(gap * gap)).astype(BF16)
                return carried

            lax.fori_loop(0, beams // 2, beam, 0, unroll=8)

    early = pairs // 2
    make_beams(range(early))
    pl.semaphore_wait(barrier, greetings)
    for c in range(len(cuts)):
        for step in range(1, slabs):
            slab_copy(c, step).start()
    make_beams(range(early, 2 * pairs))

    for c, (low, high) in enumerate(cuts):
        for step in range(1, slabs):
            slab_copy(c, step).wait_recv()
        for p in range(low, high):
            total = grad_ref[p, :, rows_of(me_s), :].astype(F32)
            for step in range(1, slabs):
                total += came[step - 1, p].astype(F32)
            gathered[me_t, p] = total.astype(WIRE)
        for step in range(1, tiles):
            tile_copy(c, step).start()

    lanes = lane_ids((slices, LANES))
    zero = jnp.zeros((slices, LANES), F32)
    for edge in (0, blocks + 1, blocks + 2):
        near[edge] = zero
        far[edge] = zero
    starts = {low: c for c, (low, high) in enumerate(cuts)}
    for p in range(pairs):
        if p in starts:
            for step in range(1, tiles):
                tile_copy(starts[p], step).wait_recv()
        for hi in range(2):
            a = p + hi * pairs
            margins = []
            for t in range(tiles):
                margin = gathered[t, p, 2 * own].astype(F32)
                margins.append(pltpu.roll(margin, HALF, 1) if hi else margin)
            for t in range(tiles):
                for b in range(own):
                    value = gathered[t, p, hi * own + b].astype(F32)
                    if b == 0 and t > 0:
                        value += jnp.where(lanes < HALO, margins[t - 1], 0.0)
                    if b == own - 1 and t + 1 < tiles:
                        value += jnp.where(lanes >= LANES - HALO, margins[t + 1], 0.0)
                    k = t * own + b + 1
                    near[k] = pltpu.roll(value, LANES - HALO, 1)
                    far[k] = pltpu.roll(value, LANES - HALO - HALF, 1)
            shift = shift_ref[a]
            for i in range(blocks):
                k = i + 1 + shift
                lower = jnp.where(lanes < LANES - HALO, near[k], near[k + 1])
                upper = jnp.where(lanes < LANES - HALO - HALF, far[k], far[k + 1])
                rows_f32[pl.ds(i, slices, stride=blocks), :] = lower
                rows_f32[pl.ds(half_rows + i, slices, stride=blocks), :] = upper
            lhs_ref[:, a * LANES : (a + 1) * LANES] = rows_f32[...].astype(BF16)
    for c in range(len(cuts)):
        for step in range(1, tiles):
            tile_copy(c, step).wait_send()
        for step in range(1, slabs):
            slab_copy(c, step).wait_send()


def back_operands(shears, tile_shift, grads, tiles, slabs, blocks, beams):
    pairs, pieces, all_rows = grads.shape[:3]
    slices = all_rows // slabs
    angles = 2 * pairs
    rows = 2 * slices * blocks
    smem = pl.BlockSpec(memory_space=pltpu.SMEM)
    vmem = pl.BlockSpec(memory_space=pltpu.VMEM)
    return pl.pallas_call(
        functools.partial(grad_kernel, tiles, slabs, blocks, beams),
        out_shape=(
            jax.ShapeDtypeStruct((rows, angles * LANES), BF16),
            jax.ShapeDtypeStruct((angles * LANES, beams * HALF), BF16),
        ),
        in_specs=[smem, smem, vmem],
        out_specs=(vmem, vmem),
        scratch_shapes=[
            pltpu.VMEM((tiles, pairs, pieces, slices, LANES), WIRE),
            pltpu.VMEM((blocks + 3, slices, LANES), F32),
            pltpu.VMEM((blocks + 3, slices, LANES), F32),
            pltpu.VMEM((rows, LANES), F32),
            pltpu.VMEM((slabs - 1, pairs, pieces, slices, LANES), WIRE),
            pltpu.SemaphoreType.DMA((slabs - 1, pairs)),
            pltpu.SemaphoreType.DMA((slabs - 1, pairs)),
            pltpu.SemaphoreType.DMA((tiles - 1, pairs)),
            pltpu.SemaphoreType.DMA((tiles - 1, pairs)),
        ],
        compiler_params=pltpu.CompilerParams(
            collective_id=1, has_side_effects=True, vmem_limit_bytes=40 * 1024 * 1024
        ),
        name="back_operands",
    )(shears, tile_shift, grads)


def frame_kernel(
    own, owner_ref, start_ref, cos_ref, sin_ref, probe_ref, measured_ref, minus_ref, plus_ref, out_ref, acc,
):
    pairs = cos_ref.shape[0]
    frames, side, unused = measured_ref.shape
    ring = own + 1
    acc[...] = jnp.zeros_like(acc)
    lanes = lane_ids((side, LANES))

    def place(member):
        angle = owner_ref[member]
        start = start_ref[member]
        start = jnp.where(start < 0, start + ring * LANES, start)
        first = start // LANES
        offset = start - first * LANES
        second = jnp.where(first + 1 == ring, 0, first + 1)
        return angle, first, second, offset

    def by_lane(value):
        return jnp.concatenate(
            [
                jnp.concatenate([value[:side, :LANES], value[side:, :LANES]], axis=1),
                jnp.concatenate([value[:side, LANES:], value[side:, LANES:]], axis=1),
            ],
            axis=0,
        )

    def wave_of(member):
        angle, first, second, offset = place(member)
        upper = jnp.where(angle >= pairs, 1, 0)
        pair = angle - upper * pairs
        outer = lanes >= offset
        turn = jnp.where(offset > 0, LANES - offset, 0)

        def window(ref):
            return pltpu.roll(jnp.where(outer, ref[pair, upper * ring + first], ref[pair, upper * ring + second]), turn, 1)

        cosine, sine = window(cos_ref), window(sin_ref)
        probe_re, probe_im = probe_ref[0], probe_ref[1]
        return probe_re * cosine - probe_im * sine, probe_re * sine + probe_im * cosine

    def add(member, grad):
        angle, first, second, offset = place(member)
        turned = pltpu.roll(grad, offset, 1)
        kept = lanes >= offset
        acc[angle, first] += jnp.where(kept, turned, 0.0)
        acc[angle, second] += jnp.where(kept, 0.0, turned)

    def residual(far, two):
        far_re, far_im = far[:side], far[side:]
        amplitude = jnp.concatenate([measured_ref[member] for member in two], axis=1).astype(F32)
        factor = 1.0 - amplitude * lax.rsqrt(far_re * far_re + far_im * far_im + SMOOTHING)
        return jnp.concatenate([(far_re * factor).astype(BF16), (far_im * factor).astype(BF16)], axis=0)

    def step(number, carried):
        duos = [(number * GROUP + 2 * duo, number * GROUP + 2 * duo + 1) for duo in range(GROUP // 2)]
        waves = [[wave_of(member) for member in two] for two in duos]
        halves = []
        for both in waves:
            stacked = jnp.concatenate(
                [jnp.concatenate([re.astype(BF16), im.astype(BF16)], axis=1) for re, im in both], axis=0
            )
            halves.append(jnp.dot(stacked, minus_ref[...], preferred_element_type=F32).astype(BF16))
        fars = [jnp.dot(plus_ref[...], by_lane(half), preferred_element_type=F32) for half in halves]
        resids = [residual(far, two) for far, two in zip(fars, duos)]
        backs = [jnp.dot(minus_ref[...], resid, preferred_element_type=F32).astype(BF16) for resid in resids]
        nears = [jnp.dot(by_lane(back), plus_ref[...], preferred_element_type=F32) for back in backs]
        for near, two, both in zip(nears, duos, waves):
            for slot, member in enumerate(two):
                wave_re, wave_im = both[slot]
                cut = slice(slot * side, (slot + 1) * side)
                add(member, near[cut, LANES:] * wave_re - near[cut, :LANES] * wave_im)
        return carried

    lax.fori_loop(0, frames // GROUP, step, 0)
    for p in range(pairs):
        for hi in range(2):
            for b in range(own):
                out_ref[p, hi * own + b] = acc[p + hi * pairs, b].astype(WIRE)
        out_ref[p, 2 * own] = halo_join(acc[p, own], acc[p + pairs, own]).astype(WIRE)


def complex_tables(length):
    indices = np.arange(length)
    phases = (indices[:, None] * indices[None, :] % length) * (2.0 * math.pi / length)
    cosine, sine = np.cos(phases), np.sin(phases)
    minus = np.block([[cosine, -sine], [sine, cosine]])
    plus = np.block([[cosine, sine], [-sine, cosine]]) / length
    return jnp.asarray(minus, BF16), jnp.asarray(plus, BF16)


def frame_gradients(owner, shift, cosine, sine, probe, measured, own):
    pairs, waves, rows, unused = cosine.shape
    smem = pl.BlockSpec(memory_space=pltpu.SMEM)
    vmem = pl.BlockSpec(memory_space=pltpu.VMEM)
    return pl.pallas_call(
        functools.partial(frame_kernel, own),
        out_shape=jax.ShapeDtypeStruct((pairs, waves - 1, rows, LANES), WIRE),
        in_specs=[smem, smem] + [vmem] * 6,
        out_specs=vmem,
        scratch_shapes=[pltpu.VMEM((2 * pairs, own + 1, rows, LANES), F32)],
        compiler_params=pltpu.CompilerParams(vmem_limit_bytes=48 * 1024 * 1024),
        name="frames",
    )(owner, shift, cosine, sine, probe, measured, *complex_tables(LANES))


def backproject_kernel(slices, blocks, beams, lhs_ref, ker_ref, out_hbm, out_ref, sems):
    groups = beams // 8
    width = 8 * HALF
    half_rows = slices * blocks
    left = lane_ids((half_rows, LANES)) < HALF

    def copy_out(group):
        return pltpu.make_async_copy(out_ref.at[:, group], out_hbm.at[:, group], sems.at[group])

    def step(group, carried):
        start = pl.multiple_of(group * width, width)
        result = jnp.dot(lhs_ref[...], ker_ref[:, pl.ds(start, width)], preferred_element_type=F32)
        for pair in range(4):
            cols = slice(pair * LANES, (pair + 1) * LANES)
            lower, upper = result[:half_rows, cols], result[half_rows:, cols]
            crossed = pltpu.roll(jnp.where(left, upper, lower), HALF, 1)
            first = jnp.where(left, lower, crossed)
            second = jnp.where(left, crossed, upper)
            for s in range(slices):
                cut = slice(s * blocks, (s + 1) * blocks)
                out_ref[s, group, pl.ds(2 * pair, blocks, stride=8), :] = first[cut]
                out_ref[s, group, pl.ds(2 * pair + 1, blocks, stride=8), :] = second[cut]
        copy_out(group).start()
        return carried

    lax.fori_loop(0, groups, step, 0, unroll=True)

    def finish(group, carried):
        copy_out(group).wait()
        return carried

    lax.fori_loop(0, groups, finish, 0)


def backproject(lhs, kernels, slices, beams, blocks):
    groups = beams // 8
    shape = (slices, groups, blocks * 8, LANES)
    result = pl.pallas_call(
        functools.partial(backproject_kernel, slices, blocks, beams),
        out_shape=jax.ShapeDtypeStruct(shape, F32),
        in_specs=[pl.BlockSpec(memory_space=pltpu.VMEM)] * 2,
        out_specs=pl.BlockSpec(memory_space=pltpu.HBM),
        scratch_shapes=[pltpu.VMEM(shape, F32), pltpu.SemaphoreType.DMA((groups,))],
        compiler_params=pltpu.CompilerParams(vmem_limit_bytes=32 * 1024 * 1024),
        name="backproject",
    )(lhs, kernels)
    result = result.reshape(slices, groups, blocks, 8, LANES).transpose(0, 1, 3, 2, 4)
    return result.reshape(slices, beams, blocks * LANES)


def body(volume, shears, tile_shift, illumination, measured, frame_owner, frame_shift):
    tiles, slabs = lax.axis_size("tile"), lax.axis_size("slab")
    slices, beams, width = volume.shape
    blocks = width // LANES
    offsets = tile_shift.reshape(-1)
    owner = frame_owner.reshape(-1)
    cosine, sine = phase_waves(shears, offsets, volume, tiles, slabs)
    grads = frame_gradients(owner, frame_shift, cosine, sine, illumination, measured, blocks // tiles)
    lhs, kernels = back_operands(shears, offsets, grads, tiles, slabs, blocks, beams)
    return backproject(lhs, kernels, slices, beams, blocks)


def solution(mesh):
    in_specs = (
        P("slab", "tile", None),
        P(),
        P(None, "tile"),
        P(),
        P(("slab", "tile"), None, None),
        P(("slab", "tile"), None),
        P(("slab", "tile")),
    )
    out_specs = P("slab", "tile", None)
    return jax.shard_map(body, mesh=mesh, in_specs=in_specs, out_specs=out_specs, check_vma=False)
```

```python
import functools
import math

import jax
import jax.numpy as jnp
import numpy as np
from jax import lax
from jax.experimental import pallas as pl
from jax.experimental.pallas import tpu as pltpu
from jax.sharding import PartitionSpec as P

LANES = 128
HALF = LANES // 2
HALO = 32
SMOOTHING = 0.25
WIRE = jnp.bfloat16
F32 = jnp.float32
BF16 = jnp.bfloat16
MESH = pl.DeviceIdType.MESH
ROOT = math.sqrt(0.5 * math.log2(math.e))
GROUP = 32
PHASE_CUTS = 4
SIN_POLY = (3.1415926401307073, -5.1677100835078775, 2.550077523214199, -0.5982912856179897, 0.07765766030124945)
COS_POLY = (0.9999999532476078, -4.934792830619626, 4.0584113528622625, -1.331876568078962, 0.2196896110945085)


def lane_ids(shape):
    return lax.broadcasted_iota(jnp.int32, shape, len(shape) - 1)


def row_ids(shape):
    return lax.broadcasted_iota(jnp.int32, shape, len(shape) - 2)


def halo_join(low, high):
    lanes = lane_ids(low.shape)
    outer = (lanes < HALO) | (lanes >= LANES - HALO)
    return jnp.where(outer, low, pltpu.roll(high, HALF, 1))


def signal_peers(axes):
    barrier = pltpu.get_barrier_semaphore()
    total = 0
    for axis, count in axes:
        me = lax.axis_index(axis)
        for step in range(1, count):
            pl.semaphore_signal(
                barrier, inc=1, device_id={axis: lax.rem(me + step, count)}, device_id_type=MESH
            )
            total += 1
    return barrier, total


def cuts_of(pairs, parts):
    ends = [pairs * part // parts for part in range(parts + 1)]
    return [(low, high) for low, high in zip(ends, ends[1:]) if low < high]


def sin_cos(phase):
    turns = phase * (0.5 / math.pi)
    turns = turns - jnp.round(turns)
    square = turns * turns
    sine, cosine = SIN_POLY[-1], COS_POLY[-1]
    for low_s, low_c in zip(SIN_POLY[-2::-1], COS_POLY[-2::-1]):
        sine = sine * square + low_s
        cosine = cosine * square + low_c
    sine = sine * turns
    double = sine + sine
    return double * cosine, 1.0 - double * sine


def phase_kernel(
    tiles, slabs, slices, beams, blocks,
    shears_hbm, shift_hbm, v_hbm, cos_ref, sin_ref,
    shears_ref, shift_ref, v_ref, lhs, ker, res, comb, parts, came, phase,
    small_sem, volume_sem, tile_send, tile_recv, slab_send, slab_recv,
):
    pairs = phase.shape[0]
    own = blocks // tiles
    groups = beams // 8
    half_rows = slices * blocks
    me_t = lax.axis_index("tile")
    me_s = lax.axis_index("slab")
    rows = pl.ds(pl.multiple_of(me_s * slices, slices), slices)

    small = [
        pltpu.make_async_copy(shears_hbm, shears_ref, small_sem.at[0]),
        pltpu.make_async_copy(shift_hbm, shift_ref, small_sem.at[1]),
    ]
    for copy in small:
        copy.start()

    def volume_copy(group):
        return pltpu.make_async_copy(v_hbm.at[:, group], v_ref.at[group], volume_sem.at[group])

    for group in range(groups):
        volume_copy(group).start()
    barrier, greetings = signal_peers((("tile", tiles), ("slab", slabs)))

    cuts = cuts_of(pairs, PHASE_CUTS)

    def tile_copy(p, step):
        peer = lax.rem(me_t + step, tiles)
        return pltpu.make_async_remote_copy(
            src_ref=parts.at[peer, p],
            dst_ref=came.at[step - 1, p],
            send_sem=tile_send.at[step - 1, p],
            recv_sem=tile_recv.at[step - 1, p],
            device_id={"tile": peer},
            device_id_type=MESH,
        )

    def slab_copy(c, step):
        low, high = cuts[c]
        return pltpu.make_async_remote_copy(
            src_ref=phase.at[low:high, :, rows, :],
            dst_ref=phase.at[low:high, :, rows, :],
            send_sem=slab_send.at[step - 1, c],
            recv_sem=slab_recv.at[step - 1, c],
            device_id={"slab": lax.rem(me_s + step, slabs)},
            device_id_type=MESH,
        )

    shape = (16, LANES)
    base = (lane_ids(shape) - row_ids(shape) - HALO).astype(F32) * ROOT
    lanes = lane_ids((half_rows, LANES))
    lanes_s = lane_ids((slices, LANES))
    zero = jnp.zeros((slices, LANES), F32)

    def make_beam_group(p, group):
        steps = [shears_ref[p] * ROOT, shears_ref[p + pairs] * ROOT]
        for beam in range(8):
            q = group * 8 + beam
            place = jnp.asarray(q, F32) - (beams - 1) * 0.5
            row = q * HALF if isinstance(q, int) else pl.multiple_of(q * HALF, HALF)
            for side in range(2):
                gap = base - place * steps[side]
                rows_of = jnp.exp2(-(gap * gap)).astype(BF16)
                for turn in range(HALF // 16):
                    turned = pltpu.roll(rows_of, 16 * turn, 1) if turn else rows_of
                    ker[p % 2, pl.ds(row + 16 * turn, 16), side * LANES : (side + 1) * LANES] = turned

    def make_beams(p):
        for group in range(groups):
            make_beam_group(p, group)

    def arrange(group, carried):
        volume_copy(group).wait()
        for pair in range(4):
            col = pl.multiple_of((group * 4 + pair) * LANES, LANES)
            for duo in range(slices // 2):
                lower, upper = [], []
                for s in (2 * duo, 2 * duo + 1):
                    first = v_ref[group, s, pl.ds(2 * pair, blocks, stride=8), :]
                    second = v_ref[group, s, pl.ds(2 * pair + 1, blocks, stride=8), :]
                    left = lane_ids(first.shape) < HALF
                    crossed = pltpu.roll(jnp.where(left, second, first), HALF, 1)
                    lower.append(jnp.where(left, first, crossed))
                    upper.append(jnp.where(left, crossed, second))
                row = 2 * duo * blocks
                lhs[row : row + 2 * blocks, pl.ds(col, LANES)] = jnp.concatenate(lower, 0).astype(BF16)
                row += half_rows
                lhs[row : row + 2 * blocks, pl.ds(col, LANES)] = jnp.concatenate(upper, 0).astype(BF16)
        return carried

    def shifted_sums(p, side):
        cols = slice(side * LANES, (side + 1) * LANES)
        near = pltpu.roll(res[0:half_rows, cols], HALO, 1)
        far = pltpu.roll(res[half_rows : 2 * half_rows, cols], HALO + HALF, 1)
        comb[side, 0] = jnp.where(lanes >= HALO, near, 0.0) + jnp.where(lanes >= HALO + HALF, far, 0.0)
        comb[side, 1] = jnp.where(lanes < HALO, near, 0.0) + jnp.where(lanes < HALO + HALF, far, 0.0)
        shift = shift_ref[p + side * pairs]
        row_of = []
        for k in range(blocks):
            total = zero
            for o in range(2):
                i = k - shift - o
                inside = (i >= 0) & (i < blocks)
                picked = comb[side, o, pl.ds(jnp.clip(i, 0, blocks - 1), slices, stride=blocks), :]
                total += jnp.where(inside, picked, 0.0)
            row_of.append(total)
        return row_of

    def project_pair(p):
        if p:
            make_beams(p)
        res[...] = jnp.dot(lhs[...], ker[p % 2], preferred_element_type=F32)
        sums = [shifted_sums(p, side) for side in range(2)]
        for t in range(tiles):
            margins = []
            for side in range(2):
                for b in range(own):
                    parts[t, p, side * own + b] = sums[side][t * own + b].astype(WIRE)
                after = sums[side][(t + 1) * own] if t + 1 < tiles else zero
                before = sums[side][t * own - 1] if t > 0 else zero
                margins.append(jnp.where(lanes_s < HALF, after, before))
            parts[t, p, 2 * own] = halo_join(margins[0], margins[1]).astype(WIRE)

    for copy in small:
        copy.wait()
    make_beams(0)
    lax.fori_loop(0, groups, arrange, 0)
    project_pair(0)
    pl.semaphore_wait(barrier, greetings)
    for p in range(pairs):
        if p:
            project_pair(p)
        for step in range(1, tiles):
            tile_copy(p, step).start()
    for c, (low, high) in enumerate(cuts):
        for p in range(low, high):
            total = parts[me_t, p].astype(F32)
            for step in range(1, tiles):
                tile_copy(p, step).wait_recv()
                total += came[step - 1, p].astype(F32)
            phase[p, :, rows, :] = total.astype(WIRE)
        for step in range(1, slabs):
            slab_copy(c, step).start()
    starts = {low: c for c, (low, high) in enumerate(cuts)}
    for p in range(pairs):
        if p in starts:
            for step in range(1, slabs):
                slab_copy(starts[p], step).wait_recv()

        def wave_piece(piece, carried):
            sine, cosine = sin_cos(phase[p, piece].astype(F32))
            place = piece + jnp.where(piece >= own, 1, 0)
            sin_ref[p, place] = sine
            cos_ref[p, place] = cosine
            return carried

        lax.fori_loop(0, 2 * own, wave_piece, 0)
        sine, cosine = sin_cos(phase[p, 2 * own].astype(F32))
        sin_ref[p, own] = sine
        cos_ref[p, own] = cosine
        sin_ref[p, 2 * own + 1] = pltpu.roll(sine, HALF, 1)
        cos_ref[p, 2 * own + 1] = pltpu.roll(cosine, HALF, 1)
    for p in range(pairs):
        for step in range(1, tiles):
            tile_copy(p, step).wait_send()
    for c in range(len(cuts)):
        for step in range(1, slabs):
            slab_copy(c, step).wait_send()


def phase_waves(shears, tile_shift, volume, tiles, slabs):
    slices, beams, width = volume.shape
    blocks = width // LANES
    angles = shears.shape[0]
    pairs, own, groups = angles // 2, blocks // tiles, beams // 8
    pieces = 2 * own + 1
    view = volume.reshape(slices, groups, 8, blocks, LANES).transpose(0, 1, 3, 2, 4)
    view = view.reshape(slices, groups, blocks * 8, LANES)
    rows = 2 * slices * blocks
    waves = jax.ShapeDtypeStruct((pairs, 2 * (own + 1), slabs * slices, LANES), F32)
    return pl.pallas_call(
        functools.partial(phase_kernel, tiles, slabs, slices, beams, blocks),
        out_shape=(waves, waves),
        in_specs=[pl.BlockSpec(memory_space=pltpu.HBM)] * 3,
        out_specs=(pl.BlockSpec(memory_space=pltpu.VMEM),) * 2,
        scratch_shapes=[
            pltpu.SMEM((angles,), F32),
            pltpu.SMEM((angles,), jnp.int32),
            pltpu.VMEM((groups, slices, blocks * 8, LANES), F32),
            pltpu.VMEM((rows, beams * HALF), BF16),
            pltpu.VMEM((2, beams * HALF, 2 * LANES), BF16),
            pltpu.VMEM((rows, 2 * LANES), F32),
            pltpu.VMEM((2, 2, rows // 2, LANES), F32),
            pltpu.VMEM((tiles, pairs, pieces, slices, LANES), WIRE),
            pltpu.VMEM((tiles - 1, pairs, pieces, slices, LANES), WIRE),
            pltpu.VMEM((pairs, pieces, slabs * slices, LANES), WIRE),
            pltpu.SemaphoreType.DMA((2,)),
            pltpu.SemaphoreType.DMA((groups,)),
            pltpu.SemaphoreType.DMA((tiles - 1, pairs)),
            pltpu.SemaphoreType.DMA((tiles - 1, pairs)),
            pltpu.SemaphoreType.DMA((slabs - 1, pairs)),
            pltpu.SemaphoreType.DMA((slabs - 1, pairs)),
        ],
        compiler_params=pltpu.CompilerParams(
            collective_id=0, has_side_effects=True, vmem_limit_bytes=40 * 1024 * 1024
        ),
        name="phase_waves",
    )(
        pltpu.with_memory_space_constraint(shears, pltpu.HBM),
        pltpu.with_memory_space_constraint(tile_shift, pltpu.HBM),
        pltpu.with_memory_space_constraint(view, pltpu.HBM),
    )


def grad_kernel(
    tiles, slabs, blocks, beams,
    shears_ref, shift_ref, grad_ref, lhs_ref, ker_ref, part_ref,
    core_came, pair_sum, came, gathered, near, far, rows_f32, old_lhs, old_ker,
    core_send, core_recv, slab_send, slab_recv, tile_send, tile_recv,
):
    pairs, pieces, chips, both_rows = grad_ref.shape[:4]
    own = (pieces - 1) // 2
    slices = both_rows // 2
    half_rows = slices * blocks
    last = pairs - 1
    me_t = lax.axis_index("tile")
    me_s = lax.axis_index("slab")
    me_chip = me_s // 2
    me_core = me_s - 2 * me_chip
    barrier, greetings = signal_peers((("tile", tiles), ("slab", slabs)))

    def rows_of(core):
        return pl.ds(pl.multiple_of(core * slices, slices), slices)

    def core_copy(p):
        return pltpu.make_async_remote_copy(
            src_ref=grad_ref.at[p, :, :, rows_of(1 - me_core), :],
            dst_ref=core_came.at[p],
            send_sem=core_send.at[p],
            recv_sem=core_recv.at[p],
            device_id={"slab": 2 * me_chip + 1 - me_core},
            device_id_type=MESH,
        )

    def slab_copy(p, step):
        peer = lax.rem(me_chip + step, chips)
        return pltpu.make_async_remote_copy(
            src_ref=pair_sum.at[p, :, peer],
            dst_ref=came.at[step - 1, p],
            send_sem=slab_send.at[step - 1, p],
            recv_sem=slab_recv.at[step - 1, p],
            device_id={"slab": 2 * peer + me_core},
            device_id_type=MESH,
        )

    def tile_copy(p, step):
        return pltpu.make_async_remote_copy(
            src_ref=gathered.at[me_t, p],
            dst_ref=gathered.at[me_t, p],
            send_sem=tile_send.at[step - 1, p],
            recv_sem=tile_recv.at[step - 1, p],
            device_id={"tile": lax.rem(me_t + step, tiles)},
            device_id_type=MESH,
        )

    shape = (LANES, LANES)
    base = (row_ids(shape) - lane_ids(shape) % HALF - HALO).astype(F32) * ROOT
    pick = (lane_ids((1, LANES)) >= HALF).astype(F32) - (beams - 1) * 0.5

    def make_beams(p):
        for hi in range(2):
            slope = shears_ref[p + hi * pairs] * ROOT
            target, row = (ker_ref, hi * LANES) if p == last else (old_ker, (2 * p + hi) * LANES)

            def beam(pair, carried):
                gap = base - (pick + (2 * pair).astype(F32)) * slope
                col = pl.multiple_of(pair * LANES, LANES)
                target[row : row + LANES, pl.ds(col, LANES)] = jnp.exp2(-(gap * gap)).astype(BF16)
                return carried

            lax.fori_loop(0, beams // 2, beam, 0, unroll=8)

    make_beams(0)
    pl.semaphore_wait(barrier, greetings)
    for p in range(pairs):
        core_copy(p).start()
    for p in range(pairs):
        core_copy(p).wait_recv()
        mine = grad_ref[p, :, :, rows_of(me_core), :].astype(F32)
        pair_sum[p] = (mine + core_came[p].astype(F32)).astype(WIRE)
        for step in range(1, chips):
            slab_copy(p, step).start()
    if pairs > 1:
        make_beams(1)
    for p in range(pairs):
        total = pair_sum[p, :, me_chip].astype(F32)
        for step in range(1, chips):
            slab_copy(p, step).wait_recv()
            total += came[step - 1, p].astype(F32)
        gathered[me_t, p] = total.astype(WIRE)
        for step in range(1, tiles):
            tile_copy(p, step).start()
    if pairs > 2:
        make_beams(2)

    lanes = lane_ids((slices, LANES))
    zero = jnp.zeros((slices, LANES), F32)
    for edge in (0, blocks + 1, blocks + 2):
        near[edge] = zero
        far[edge] = zero

    def left_operand(p):
        for hi in range(2):
            margins = []
            for t in range(tiles):
                margin = gathered[t, p, 2 * own].astype(F32)
                margins.append(pltpu.roll(margin, HALF, 1) if hi else margin)
            for t in range(tiles):
                for b in range(own):
                    value = gathered[t, p, hi * own + b].astype(F32)
                    if b == 0 and t > 0:
                        value += jnp.where(lanes < HALO, margins[t - 1], 0.0)
                    if b == own - 1 and t + 1 < tiles:
                        value += jnp.where(lanes >= LANES - HALO, margins[t + 1], 0.0)
                    k = t * own + b + 1
                    near[k] = pltpu.roll(value, LANES - HALO, 1)
                    far[k] = pltpu.roll(value, LANES - HALO - HALF, 1)
            shift = shift_ref[p + hi * pairs]
            for i in range(blocks):
                k = i + 1 + shift
                lower = jnp.where(lanes < LANES - HALO, near[k], near[k + 1])
                upper = jnp.where(lanes < LANES - HALO - HALF, far[k], far[k + 1])
                rows_f32[pl.ds(i, slices, stride=blocks), :] = lower
                rows_f32[pl.ds(half_rows + i, slices, stride=blocks), :] = upper
            target, col = (lhs_ref, hi * LANES) if p == last else (old_lhs, (2 * p + hi) * LANES)
            target[:, col : col + LANES] = rows_f32[...].astype(BF16)

    def product(low, high):
        depth = slice(2 * low * LANES, 2 * high * LANES)
        width = 8 * HALF
        for group in range(beams // 8):
            span = slice(group * width, (group + 1) * width)
            update = jnp.dot(old_lhs[:, depth], old_ker[depth, span], preferred_element_type=F32)
            if low == 0:
                part_ref[:, span] = update
            else:
                part_ref[:, span] += update

    early = max(1, last - 1)
    for p in range(pairs):
        for step in range(1, tiles):
            tile_copy(p, step).wait_recv()
        left_operand(p)
        if p + 3 < pairs:
            make_beams(p + 3)
        if p == early - 1:
            product(0, early)
        elif early <= p < last:
            product(p, p + 1)
    for p in range(pairs):
        core_copy(p).wait_send()
        for step in range(1, tiles):
            tile_copy(p, step).wait_send()
        for step in range(1, chips):
            slab_copy(p, step).wait_send()


def back_operands(shears, tile_shift, grads, tiles, slabs, blocks, beams):
    pairs, pieces, chips, both_rows = grads.shape[:4]
    slices = both_rows // 2
    rows = 2 * slices * blocks
    older = 2 * (pairs - 1) * LANES
    smem = pl.BlockSpec(memory_space=pltpu.SMEM)
    vmem = pl.BlockSpec(memory_space=pltpu.VMEM)
    return pl.pallas_call(
        functools.partial(grad_kernel, tiles, slabs, blocks, beams),
        out_shape=(
            jax.ShapeDtypeStruct((rows, 2 * LANES), BF16),
            jax.ShapeDtypeStruct((2 * LANES, beams * HALF), BF16),
            jax.ShapeDtypeStruct((rows, beams * HALF), F32),
        ),
        in_specs=[smem, smem, vmem],
        out_specs=(vmem, vmem, vmem),
        scratch_shapes=[
            pltpu.VMEM((pairs, pieces, chips, slices, LANES), WIRE),
            pltpu.VMEM((pairs, pieces, chips, slices, LANES), WIRE),
            pltpu.VMEM((chips - 1, pairs, pieces, slices, LANES), WIRE),
            pltpu.VMEM((tiles, pairs, pieces, slices, LANES), WIRE),
            pltpu.VMEM((blocks + 3, slices, LANES), F32),
            pltpu.VMEM((blocks + 3, slices, LANES), F32),
            pltpu.VMEM((rows, LANES), F32),
            pltpu.VMEM((rows, older), BF16),
            pltpu.VMEM((older, beams * HALF), BF16),
            pltpu.SemaphoreType.DMA((pairs,)),
            pltpu.SemaphoreType.DMA((pairs,)),
            pltpu.SemaphoreType.DMA((chips - 1, pairs)),
            pltpu.SemaphoreType.DMA((chips - 1, pairs)),
            pltpu.SemaphoreType.DMA((tiles - 1, pairs)),
            pltpu.SemaphoreType.DMA((tiles - 1, pairs)),
        ],
        compiler_params=pltpu.CompilerParams(
            collective_id=1, has_side_effects=True, vmem_limit_bytes=40 * 1024 * 1024
        ),
        name="back_operands",
    )(shears, tile_shift, grads)


def frame_kernel(
    own, owner_ref, start_ref, cos_ref, sin_ref, probe_ref, measured_ref, minus_ref, plus_ref, out_ref, acc,
):
    pairs = cos_ref.shape[0]
    frames, side, unused = measured_ref.shape
    ring = own + 1
    acc[...] = jnp.zeros_like(acc)
    lanes = lane_ids((side, LANES))

    def place(member):
        angle = owner_ref[member]
        start = start_ref[member]
        start = jnp.where(start < 0, start + ring * LANES, start)
        first = start // LANES
        offset = start - first * LANES
        second = jnp.where(first + 1 == ring, 0, first + 1)
        return angle, first, second, offset

    def by_lane(value):
        return jnp.concatenate(
            [
                jnp.concatenate([value[:side, :LANES], value[side:, :LANES]], axis=1),
                jnp.concatenate([value[:side, LANES:], value[side:, LANES:]], axis=1),
            ],
            axis=0,
        )

    def wave_of(member):
        angle, first, second, offset = place(member)
        upper = jnp.where(angle >= pairs, 1, 0)
        pair = angle - upper * pairs
        outer = lanes >= offset
        turn = jnp.where(offset > 0, LANES - offset, 0)

        def window(ref):
            return pltpu.roll(jnp.where(outer, ref[pair, upper * ring + first], ref[pair, upper * ring + second]), turn, 1)

        cosine, sine = window(cos_ref), window(sin_ref)
        probe_re, probe_im = probe_ref[0], probe_ref[1]
        return probe_re * cosine - probe_im * sine, probe_re * sine + probe_im * cosine

    def add(member, grad):
        angle, first, second, offset = place(member)
        turned = pltpu.roll(grad, offset, 1)
        kept = lanes >= offset
        acc[angle, first] += jnp.where(kept, turned, 0.0)
        acc[angle, second] += jnp.where(kept, 0.0, turned)

    def residual(far, two):
        far_re, far_im = far[:side], far[side:]
        amplitude = jnp.concatenate([measured_ref[member] for member in two], axis=1).astype(F32)
        factor = 1.0 - amplitude * lax.rsqrt(far_re * far_re + far_im * far_im + SMOOTHING)
        return jnp.concatenate([(far_re * factor).astype(BF16), (far_im * factor).astype(BF16)], axis=0)

    def step(number, carried):
        duos = [(number * GROUP + 2 * duo, number * GROUP + 2 * duo + 1) for duo in range(GROUP // 2)]
        waves = [[wave_of(member) for member in two] for two in duos]
        halves = []
        for both in waves:
            stacked = jnp.concatenate(
                [jnp.concatenate([re.astype(BF16), im.astype(BF16)], axis=1) for re, im in both], axis=0
            )
            halves.append(jnp.dot(stacked, minus_ref[...], preferred_element_type=F32).astype(BF16))
        fars = [jnp.dot(plus_ref[...], by_lane(half), preferred_element_type=F32) for half in halves]
        resids = [residual(far, two) for far, two in zip(fars, duos)]
        backs = [jnp.dot(minus_ref[...], resid, preferred_element_type=F32).astype(BF16) for resid in resids]
        nears = [jnp.dot(by_lane(back), plus_ref[...], preferred_element_type=F32) for back in backs]
        for near, two, both in zip(nears, duos, waves):
            for slot, member in enumerate(two):
                wave_re, wave_im = both[slot]
                cut = slice(slot * side, (slot + 1) * side)
                add(member, near[cut, LANES:] * wave_re - near[cut, :LANES] * wave_im)
        return carried

    lax.fori_loop(0, frames // GROUP, step, 0)
    for p in range(pairs):
        for hi in range(2):
            for b in range(own):
                out_ref[p, hi * own + b] = acc[p + hi * pairs, b].astype(WIRE).reshape(out_ref.shape[2:])
        out_ref[p, 2 * own] = halo_join(acc[p, own], acc[p + pairs, own]).astype(WIRE).reshape(out_ref.shape[2:])


def complex_tables(length):
    indices = np.arange(length)
    phases = (indices[:, None] * indices[None, :] % length) * (2.0 * math.pi / length)
    cosine, sine = np.cos(phases), np.sin(phases)
    minus = np.block([[cosine, -sine], [sine, cosine]])
    plus = np.block([[cosine, sine], [-sine, cosine]]) / length
    return jnp.asarray(minus, BF16), jnp.asarray(plus, BF16)


def frame_gradients(owner, shift, cosine, sine, probe, measured, own, chips):
    pairs, waves, rows, unused = cosine.shape
    smem = pl.BlockSpec(memory_space=pltpu.SMEM)
    vmem = pl.BlockSpec(memory_space=pltpu.VMEM)
    return pl.pallas_call(
        functools.partial(frame_kernel, own),
        out_shape=jax.ShapeDtypeStruct((pairs, waves - 1, chips, rows // chips, LANES), WIRE),
        in_specs=[smem, smem] + [vmem] * 6,
        out_specs=vmem,
        scratch_shapes=[pltpu.VMEM((2 * pairs, own + 1, rows, LANES), F32)],
        compiler_params=pltpu.CompilerParams(vmem_limit_bytes=48 * 1024 * 1024),
        name="frames",
    )(owner, shift, cosine, sine, probe, measured, *complex_tables(LANES))


def backproject_kernel(slices, blocks, beams, lhs_ref, ker_ref, part_ref, out_hbm, out_ref, sems):
    groups = beams // 8
    width = 8 * HALF
    half_rows = slices * blocks
    left = lane_ids((half_rows, LANES)) < HALF

    def copy_out(group):
        return pltpu.make_async_copy(out_ref.at[:, group], out_hbm.at[:, group], sems.at[group])

    def step(group, carried):
        start = pl.multiple_of(group * width, width)
        span = pl.ds(start, width)
        result = part_ref[:, span] + jnp.dot(lhs_ref[...], ker_ref[:, span], preferred_element_type=F32)
        for pair in range(4):
            cols = slice(pair * LANES, (pair + 1) * LANES)
            lower, upper = result[:half_rows, cols], result[half_rows:, cols]
            crossed = pltpu.roll(jnp.where(left, upper, lower), HALF, 1)
            first = jnp.where(left, lower, crossed)
            second = jnp.where(left, crossed, upper)
            for s in range(slices):
                cut = slice(s * blocks, (s + 1) * blocks)
                out_ref[s, group, pl.ds(2 * pair, blocks, stride=8), :] = first[cut]
                out_ref[s, group, pl.ds(2 * pair + 1, blocks, stride=8), :] = second[cut]
        copy_out(group).start()
        return carried

    lax.fori_loop(0, groups, step, 0, unroll=True)

    def finish(group, carried):
        copy_out(group).wait()
        return carried

    lax.fori_loop(0, groups, finish, 0)


def backproject(lhs, kernels, partial_sum, slices, beams, blocks):
    groups = beams // 8
    shape = (slices, groups, blocks * 8, LANES)
    result = pl.pallas_call(
        functools.partial(backproject_kernel, slices, blocks, beams),
        out_shape=jax.ShapeDtypeStruct(shape, F32),
        in_specs=[pl.BlockSpec(memory_space=pltpu.VMEM)] * 3,
        out_specs=pl.BlockSpec(memory_space=pltpu.HBM),
        scratch_shapes=[pltpu.VMEM(shape, F32), pltpu.SemaphoreType.DMA((groups,))],
        compiler_params=pltpu.CompilerParams(vmem_limit_bytes=32 * 1024 * 1024),
        name="backproject",
    )(lhs, kernels, partial_sum)
    result = result.reshape(slices, groups, blocks, 8, LANES).transpose(0, 1, 3, 2, 4)
    return result.reshape(slices, beams, blocks * LANES)


def body(volume, shears, tile_shift, illumination, measured, frame_owner, frame_shift):
    tiles, slabs = lax.axis_size("tile"), lax.axis_size("slab")
    slices, beams, width = volume.shape
    blocks = width // LANES
    offsets = tile_shift.reshape(-1)
    owner = frame_owner.reshape(-1)
    cosine, sine = phase_waves(shears, offsets, volume, tiles, slabs)
    grads = frame_gradients(owner, frame_shift, cosine, sine, illumination, measured, blocks // tiles, slabs // 2)
    lhs, kernels, partial_sum = back_operands(shears, offsets, grads, tiles, slabs, blocks, beams)
    return backproject(lhs, kernels, partial_sum, slices, beams, blocks)


def solution(mesh):
    in_specs = (
        P("slab", "tile", None),
        P(),
        P(None, "tile"),
        P(),
        P(("slab", "tile"), None, None),
        P(("slab", "tile"), None),
        P(("slab", "tile")),
    )
    out_specs = P("slab", "tile", None)
    return jax.shard_map(body, mesh=mesh, in_specs=in_specs, out_specs=out_specs, check_vma=False)
```

```python
import functools
import math

import jax
import jax.numpy as jnp
import numpy as np
from jax import lax
from jax.experimental import pallas as pl
from jax.experimental.pallas import tpu as pltpu
from jax.sharding import PartitionSpec as P

LANES = 128
HALF = LANES // 2
HALO = 32
SMOOTHING = 0.25
WIRE = jnp.bfloat16
F32 = jnp.float32
BF16 = jnp.bfloat16
MESH = pl.DeviceIdType.MESH
ROOT = math.sqrt(0.5 * math.log2(math.e))
GROUP = 32
PHASE_CUTS = 4
SIN_POLY = (3.1415926401307073, -5.1677100835078775, 2.550077523214199, -0.5982912856179897, 0.07765766030124945)
COS_POLY = (0.9999999532476078, -4.934792830619626, 4.0584113528622625, -1.331876568078962, 0.2196896110945085)


def lane_ids(shape):
    return lax.broadcasted_iota(jnp.int32, shape, len(shape) - 1)


def row_ids(shape):
    return lax.broadcasted_iota(jnp.int32, shape, len(shape) - 2)


def halo_join(low, high):
    lanes = lane_ids(low.shape)
    outer = (lanes < HALO) | (lanes >= LANES - HALO)
    return jnp.where(outer, low, pltpu.roll(high, HALF, 1))


def signal_peers(axes):
    barrier = pltpu.get_barrier_semaphore()
    total = 0
    for axis, count in axes:
        me = lax.axis_index(axis)
        for step in range(1, count):
            pl.semaphore_signal(
                barrier, inc=1, device_id={axis: lax.rem(me + step, count)}, device_id_type=MESH
            )
            total += 1
    return barrier, total


def cuts_of(pairs, parts):
    ends = [pairs * part // parts for part in range(parts + 1)]
    return [(low, high) for low, high in zip(ends, ends[1:]) if low < high]


def sin_cos(phase):
    turns = phase * (0.5 / math.pi)
    turns = turns - jnp.round(turns)
    square = turns * turns
    sine, cosine = SIN_POLY[-1], COS_POLY[-1]
    for low_s, low_c in zip(SIN_POLY[-2::-1], COS_POLY[-2::-1]):
        sine = sine * square + low_s
        cosine = cosine * square + low_c
    sine = sine * turns
    double = sine + sine
    return double * cosine, 1.0 - double * sine


def phase_kernel(
    tiles, slabs, slices, beams, blocks,
    shears_hbm, shift_hbm, v_hbm, cos_ref, sin_ref,
    shears_ref, shift_ref, v_ref, lhs, ker, res, comb, parts, came, phase,
    small_sem, volume_sem, tile_send, tile_recv, slab_send, slab_recv,
):
    pairs = phase.shape[0]
    own = blocks // tiles
    groups = beams // 8
    half_rows = slices * blocks
    me_t = lax.axis_index("tile")
    me_s = lax.axis_index("slab")
    rows = pl.ds(pl.multiple_of(me_s * slices, slices), slices)

    small = [
        pltpu.make_async_copy(shears_hbm, shears_ref, small_sem.at[0]),
        pltpu.make_async_copy(shift_hbm, shift_ref, small_sem.at[1]),
    ]
    for copy in small:
        copy.start()

    def volume_copy(group):
        return pltpu.make_async_copy(v_hbm.at[:, group], v_ref.at[group], volume_sem.at[group])

    for group in range(groups):
        volume_copy(group).start()
    barrier, greetings = signal_peers((("tile", tiles), ("slab", slabs)))

    cuts = cuts_of(pairs, PHASE_CUTS)

    def tile_copy(p, step):
        peer = lax.rem(me_t + step, tiles)
        return pltpu.make_async_remote_copy(
            src_ref=parts.at[peer, p],
            dst_ref=came.at[step - 1, p],
            send_sem=tile_send.at[step - 1, p],
            recv_sem=tile_recv.at[step - 1, p],
            device_id={"tile": peer},
            device_id_type=MESH,
        )

    def slab_copy(c, step):
        low, high = cuts[c]
        return pltpu.make_async_remote_copy(
            src_ref=phase.at[low:high, :, rows, :],
            dst_ref=phase.at[low:high, :, rows, :],
            send_sem=slab_send.at[step - 1, c],
            recv_sem=slab_recv.at[step - 1, c],
            device_id={"slab": lax.rem(me_s + step, slabs)},
            device_id_type=MESH,
        )

    shape = (16, LANES)
    base = (lane_ids(shape) - row_ids(shape) - HALO).astype(F32) * ROOT
    lanes = lane_ids((half_rows, LANES))
    lanes_s = lane_ids((slices, LANES))
    zero = jnp.zeros((slices, LANES), F32)

    def make_beam_group(p, group):
        steps = [shears_ref[p] * ROOT, shears_ref[p + pairs] * ROOT]
        for beam in range(8):
            q = group * 8 + beam
            place = jnp.asarray(q, F32) - (beams - 1) * 0.5
            row = q * HALF if isinstance(q, int) else pl.multiple_of(q * HALF, HALF)
            for side in range(2):
                gap = base - place * steps[side]
                rows_of = jnp.exp2(-(gap * gap)).astype(BF16)
                for turn in range(HALF // 16):
                    turned = pltpu.roll(rows_of, 16 * turn, 1) if turn else rows_of
                    ker[p % 2, pl.ds(row + 16 * turn, 16), side * LANES : (side + 1) * LANES] = turned

    def make_beams(p):
        for group in range(groups):
            make_beam_group(p, group)

    def arrange(group):
        volume_copy(group).wait()
        for pair in range(4):
            col = (group * 4 + pair) * LANES
            for duo in range(slices // 2):
                lower, upper = [], []
                for s in (2 * duo, 2 * duo + 1):
                    first = v_ref[group, s, pl.ds(2 * pair, blocks, stride=8), :]
                    second = v_ref[group, s, pl.ds(2 * pair + 1, blocks, stride=8), :]
                    left = lane_ids(first.shape) < HALF
                    crossed = pltpu.roll(jnp.where(left, second, first), HALF, 1)
                    lower.append(jnp.where(left, first, crossed))
                    upper.append(jnp.where(left, crossed, second))
                row = 2 * duo * blocks
                lhs[row : row + 2 * blocks, col : col + LANES] = jnp.concatenate(lower, 0).astype(BF16)
                row += half_rows
                lhs[row : row + 2 * blocks, col : col + LANES] = jnp.concatenate(upper, 0).astype(BF16)

    def shifted_sums(p, side):
        cols = slice(side * LANES, (side + 1) * LANES)
        near = pltpu.roll(res[0:half_rows, cols], HALO, 1)
        far = pltpu.roll(res[half_rows : 2 * half_rows, cols], HALO + HALF, 1)
        comb[side, 0] = jnp.where(lanes >= HALO, near, 0.0) + jnp.where(lanes >= HALO + HALF, far, 0.0)
        comb[side, 1] = jnp.where(lanes < HALO, near, 0.0) + jnp.where(lanes < HALO + HALF, far, 0.0)
        shift = shift_ref[p + side * pairs]
        row_of = []
        for k in range(blocks):
            total = zero
            for o in range(2):
                i = k - shift - o
                inside = (i >= 0) & (i < blocks)
                picked = comb[side, o, pl.ds(jnp.clip(i, 0, blocks - 1), slices, stride=blocks), :]
                total += jnp.where(inside, picked, 0.0)
            row_of.append(total)
        return row_of

    def project_pair(p):
        if p:
            make_beams(p)
        res[...] = jnp.dot(lhs[...], ker[p % 2], preferred_element_type=F32)
        sums = [shifted_sums(p, side) for side in range(2)]
        for t in range(tiles):
            margins = []
            for side in range(2):
                for b in range(own):
                    parts[t, p, side * own + b] = sums[side][t * own + b].astype(WIRE)
                after = sums[side][(t + 1) * own] if t + 1 < tiles else zero
                before = sums[side][t * own - 1] if t > 0 else zero
                margins.append(jnp.where(lanes_s < HALF, after, before))
            parts[t, p, 2 * own] = halo_join(margins[0], margins[1]).astype(WIRE)

    for copy in small:
        copy.wait()
    make_beams(0)
    for group in range(groups):
        arrange(group)
    project_pair(0)
    pl.semaphore_wait(barrier, greetings)
    for p in range(pairs):
        if p:
            project_pair(p)
        for step in range(1, tiles):
            tile_copy(p, step).start()
    for c, (low, high) in enumerate(cuts):
        for p in range(low, high):
            total = parts[me_t, p].astype(F32)
            for step in range(1, tiles):
                tile_copy(p, step).wait_recv()
                total += came[step - 1, p].astype(F32)
            phase[p, :, rows, :] = total.astype(WIRE)
        for step in range(1, slabs):
            slab_copy(c, step).start()
    starts = {low: c for c, (low, high) in enumerate(cuts)}
    for p in range(pairs):
        if p in starts:
            for step in range(1, slabs):
                slab_copy(starts[p], step).wait_recv()

        def wave_piece(piece, carried):
            sine, cosine = sin_cos(phase[p, piece].astype(F32))
            place = piece + jnp.where(piece >= own, 1, 0)
            sin_ref[p, place] = sine
            cos_ref[p, place] = cosine
            return carried

        lax.fori_loop(0, 2 * own, wave_piece, 0)
        sine, cosine = sin_cos(phase[p, 2 * own].astype(F32))
        sin_ref[p, own] = sine
        cos_ref[p, own] = cosine
        sin_ref[p, 2 * own + 1] = pltpu.roll(sine, HALF, 1)
        cos_ref[p, 2 * own + 1] = pltpu.roll(cosine, HALF, 1)
    for p in range(pairs):
        for step in range(1, tiles):
            tile_copy(p, step).wait_send()
    for c in range(len(cuts)):
        for step in range(1, slabs):
            slab_copy(c, step).wait_send()


def phase_waves(shears, tile_shift, volume, tiles, slabs):
    slices, beams, width = volume.shape
    blocks = width // LANES
    angles = shears.shape[0]
    pairs, own, groups = angles // 2, blocks // tiles, beams // 8
    pieces = 2 * own + 1
    view = volume.reshape(slices, groups, 8, blocks, LANES).transpose(0, 1, 3, 2, 4)
    view = view.reshape(slices, groups, blocks * 8, LANES)
    rows = 2 * slices * blocks
    waves = jax.ShapeDtypeStruct((pairs, 2 * (own + 1), slabs * slices, LANES), F32)
    return pl.pallas_call(
        functools.partial(phase_kernel, tiles, slabs, slices, beams, blocks),
        out_shape=(waves, waves),
        in_specs=[pl.BlockSpec(memory_space=pltpu.HBM)] * 3,
        out_specs=(pl.BlockSpec(memory_space=pltpu.VMEM),) * 2,
        scratch_shapes=[
            pltpu.SMEM((angles,), F32),
            pltpu.SMEM((angles,), jnp.int32),
            pltpu.VMEM((groups, slices, blocks * 8, LANES), F32),
            pltpu.VMEM((rows, beams * HALF), BF16),
            pltpu.VMEM((2, beams * HALF, 2 * LANES), BF16),
            pltpu.VMEM((rows, 2 * LANES), F32),
            pltpu.VMEM((2, 2, rows // 2, LANES), F32),
            pltpu.VMEM((tiles, pairs, pieces, slices, LANES), WIRE),
            pltpu.VMEM((tiles - 1, pairs, pieces, slices, LANES), WIRE),
            pltpu.VMEM((pairs, pieces, slabs * slices, LANES), WIRE),
            pltpu.SemaphoreType.DMA((2,)),
            pltpu.SemaphoreType.DMA((groups,)),
            pltpu.SemaphoreType.DMA((tiles - 1, pairs)),
            pltpu.SemaphoreType.DMA((tiles - 1, pairs)),
            pltpu.SemaphoreType.DMA((slabs - 1, pairs)),
            pltpu.SemaphoreType.DMA((slabs - 1, pairs)),
        ],
        compiler_params=pltpu.CompilerParams(
            collective_id=0, has_side_effects=True, vmem_limit_bytes=40 * 1024 * 1024
        ),
        name="phase_waves",
    )(
        pltpu.with_memory_space_constraint(shears, pltpu.HBM),
        pltpu.with_memory_space_constraint(tile_shift, pltpu.HBM),
        pltpu.with_memory_space_constraint(view, pltpu.HBM),
    )


def grad_kernel(
    tiles, slabs, blocks, beams,
    shears_ref, shift_ref, grad_ref, lhs_ref, ker_ref, part_ref,
    core_came, pair_sum, came, gathered, near, far, rows_f32, old_lhs, old_ker,
    core_send, core_recv, slab_send, slab_recv, tile_send, tile_recv,
):
    pairs, pieces, chips, both_rows = grad_ref.shape[:4]
    own = (pieces - 1) // 2
    slices = both_rows // 2
    half_rows = slices * blocks
    last = pairs - 1
    me_t = lax.axis_index("tile")
    me_s = lax.axis_index("slab")
    me_chip = me_s // 2
    me_core = me_s - 2 * me_chip
    barrier, greetings = signal_peers((("tile", tiles), ("slab", slabs)))

    def rows_of(core):
        return pl.ds(pl.multiple_of(core * slices, slices), slices)

    def core_copy(p):
        return pltpu.make_async_remote_copy(
            src_ref=grad_ref.at[p, :, :, rows_of(1 - me_core), :],
            dst_ref=core_came.at[p],
            send_sem=core_send.at[p],
            recv_sem=core_recv.at[p],
            device_id={"slab": 2 * me_chip + 1 - me_core},
            device_id_type=MESH,
        )

    def slab_copy(p, step):
        peer = lax.rem(me_chip + step, chips)
        return pltpu.make_async_remote_copy(
            src_ref=pair_sum.at[p, :, peer],
            dst_ref=came.at[step - 1, p],
            send_sem=slab_send.at[step - 1, p],
            recv_sem=slab_recv.at[step - 1, p],
            device_id={"slab": 2 * peer + me_core},
            device_id_type=MESH,
        )

    def tile_copy(p, step):
        return pltpu.make_async_remote_copy(
            src_ref=gathered.at[me_t, p],
            dst_ref=gathered.at[me_t, p],
            send_sem=tile_send.at[step - 1, p],
            recv_sem=tile_recv.at[step - 1, p],
            device_id={"tile": lax.rem(me_t + step, tiles)},
            device_id_type=MESH,
        )

    shape = (LANES, LANES)
    base = (row_ids(shape) - lane_ids(shape) % HALF - HALO).astype(F32) * ROOT
    pick = (lane_ids((1, LANES)) >= HALF).astype(F32) - (beams - 1) * 0.5

    def make_beams(p):
        for hi in range(2):
            slope = shears_ref[p + hi * pairs] * ROOT
            target, row = (ker_ref, hi * LANES) if p == last else (old_ker, (2 * p + hi) * LANES)

            def beam(pair, carried):
                gap = base - (pick + (2 * pair).astype(F32)) * slope
                col = pl.multiple_of(pair * LANES, LANES)
                target[row : row + LANES, pl.ds(col, LANES)] = jnp.exp2(-(gap * gap)).astype(BF16)
                return carried

            lax.fori_loop(0, beams // 2, beam, 0, unroll=8)

    make_beams(0)
    pl.semaphore_wait(barrier, greetings)
    for p in range(pairs):
        core_copy(p).start()
    for p in range(pairs):
        core_copy(p).wait_recv()
        mine = grad_ref[p, :, :, rows_of(me_core), :].astype(F32)
        pair_sum[p] = (mine + core_came[p].astype(F32)).astype(WIRE)
        for step in range(1, chips):
            slab_copy(p, step).start()
    if pairs > 1:
        make_beams(1)
    for p in range(pairs):
        total = pair_sum[p, :, me_chip].astype(F32)
        for step in range(1, chips):
            slab_copy(p, step).wait_recv()
            total += came[step - 1, p].astype(F32)
        gathered[me_t, p] = total.astype(WIRE)
        for step in range(1, tiles):
            tile_copy(p, step).start()
    if pairs > 2:
        make_beams(2)

    lanes = lane_ids((slices, LANES))
    zero = jnp.zeros((slices, LANES), F32)
    for edge in (0, blocks + 1, blocks + 2):
        near[edge] = zero
        far[edge] = zero

    def left_operand(p):
        for hi in range(2):
            margins = []
            for t in range(tiles):
                margin = gathered[t, p, 2 * own].astype(F32)
                margins.append(pltpu.roll(margin, HALF, 1) if hi else margin)
            for t in range(tiles):
                for b in range(own):
                    value = gathered[t, p, hi * own + b].astype(F32)
                    if b == 0 and t > 0:
                        value += jnp.where(lanes < HALO, margins[t - 1], 0.0)
                    if b == own - 1 and t + 1 < tiles:
                        value += jnp.where(lanes >= LANES - HALO, margins[t + 1], 0.0)
                    k = t * own + b + 1
                    near[k] = pltpu.roll(value, LANES - HALO, 1)
                    far[k] = pltpu.roll(value, LANES - HALO - HALF, 1)
            shift = shift_ref[p + hi * pairs]
            for i in range(blocks):
                k = i + 1 + shift
                lower = jnp.where(lanes < LANES - HALO, near[k], near[k + 1])
                upper = jnp.where(lanes < LANES - HALO - HALF, far[k], far[k + 1])
                rows_f32[pl.ds(i, slices, stride=blocks), :] = lower
                rows_f32[pl.ds(half_rows + i, slices, stride=blocks), :] = upper
            target, col = (lhs_ref, hi * LANES) if p == last else (old_lhs, (2 * p + hi) * LANES)
            target[:, col : col + LANES] = rows_f32[...].astype(BF16)

    def product(low, high):
        depth = slice(2 * low * LANES, 2 * high * LANES)
        width = 8 * HALF
        for group in range(beams // 8):
            span = slice(group * width, (group + 1) * width)
            update = jnp.dot(old_lhs[:, depth], old_ker[depth, span], preferred_element_type=F32)
            if low == 0:
                part_ref[:, span] = update
            else:
                part_ref[:, span] += update

    early = max(1, last - 1)
    for p in range(pairs):
        for step in range(1, tiles):
            tile_copy(p, step).wait_recv()
        left_operand(p)
        if p + 3 < pairs:
            make_beams(p + 3)
        if p == early - 1:
            product(0, early)
        elif early <= p < last:
            product(p, p + 1)
    for p in range(pairs):
        core_copy(p).wait_send()
        for step in range(1, tiles):
            tile_copy(p, step).wait_send()
        for step in range(1, chips):
            slab_copy(p, step).wait_send()


def back_operands(shears, tile_shift, grads, tiles, slabs, blocks, beams):
    pairs, pieces, chips, both_rows = grads.shape[:4]
    slices = both_rows // 2
    rows = 2 * slices * blocks
    older = 2 * (pairs - 1) * LANES
    smem = pl.BlockSpec(memory_space=pltpu.SMEM)
    vmem = pl.BlockSpec(memory_space=pltpu.VMEM)
    return pl.pallas_call(
        functools.partial(grad_kernel, tiles, slabs, blocks, beams),
        out_shape=(
            jax.ShapeDtypeStruct((rows, 2 * LANES), BF16),
            jax.ShapeDtypeStruct((2 * LANES, beams * HALF), BF16),
            jax.ShapeDtypeStruct((rows, beams * HALF), F32),
        ),
        in_specs=[smem, smem, vmem],
        out_specs=(vmem, vmem, vmem),
        scratch_shapes=[
            pltpu.VMEM((pairs, pieces, chips, slices, LANES), WIRE),
            pltpu.VMEM((pairs, pieces, chips, slices, LANES), WIRE),
            pltpu.VMEM((chips - 1, pairs, pieces, slices, LANES), WIRE),
            pltpu.VMEM((tiles, pairs, pieces, slices, LANES), WIRE),
            pltpu.VMEM((blocks + 3, slices, LANES), F32),
            pltpu.VMEM((blocks + 3, slices, LANES), F32),
            pltpu.VMEM((rows, LANES), F32),
            pltpu.VMEM((rows, older), BF16),
            pltpu.VMEM((older, beams * HALF), BF16),
            pltpu.SemaphoreType.DMA((pairs,)),
            pltpu.SemaphoreType.DMA((pairs,)),
            pltpu.SemaphoreType.DMA((chips - 1, pairs)),
            pltpu.SemaphoreType.DMA((chips - 1, pairs)),
            pltpu.SemaphoreType.DMA((tiles - 1, pairs)),
            pltpu.SemaphoreType.DMA((tiles - 1, pairs)),
        ],
        compiler_params=pltpu.CompilerParams(
            collective_id=1, has_side_effects=True, vmem_limit_bytes=40 * 1024 * 1024
        ),
        name="back_operands",
    )(shears, tile_shift, grads)


def frame_kernel(
    own, owner_ref, start_ref, cos_ref, sin_ref, probe_ref, measured_ref, minus_ref, plus_ref, out_ref, acc,
):
    pairs = cos_ref.shape[0]
    frames, side, unused = measured_ref.shape
    ring = own + 1
    acc[...] = jnp.zeros_like(acc)
    lanes = lane_ids((side, LANES))

    def place(member):
        angle = owner_ref[member]
        start = start_ref[member]
        start = jnp.where(start < 0, start + ring * LANES, start)
        first = start // LANES
        offset = start - first * LANES
        second = jnp.where(first + 1 == ring, 0, first + 1)
        return angle, first, second, offset

    def by_lane(value):
        return jnp.concatenate(
            [
                jnp.concatenate([value[:side, :LANES], value[side:, :LANES]], axis=1),
                jnp.concatenate([value[:side, LANES:], value[side:, LANES:]], axis=1),
            ],
            axis=0,
        )

    def wave_of(member):
        angle, first, second, offset = place(member)
        upper = jnp.where(angle >= pairs, 1, 0)
        pair = angle - upper * pairs
        outer = lanes >= offset
        turn = jnp.where(offset > 0, LANES - offset, 0)

        def window(ref):
            return pltpu.roll(jnp.where(outer, ref[pair, upper * ring + first], ref[pair, upper * ring + second]), turn, 1)

        cosine, sine = window(cos_ref), window(sin_ref)
        probe_re, probe_im = probe_ref[0], probe_ref[1]
        return probe_re * cosine - probe_im * sine, probe_re * sine + probe_im * cosine

    def add(member, grad):
        angle, first, second, offset = place(member)
        turned = pltpu.roll(grad, offset, 1)
        kept = lanes >= offset
        acc[angle, first] += jnp.where(kept, turned, 0.0)
        acc[angle, second] += jnp.where(kept, 0.0, turned)

    def residual(far, two):
        far_re, far_im = far[:side], far[side:]
        amplitude = jnp.concatenate([measured_ref[member] for member in two], axis=1).astype(F32)
        factor = 1.0 - amplitude * lax.rsqrt(far_re * far_re + far_im * far_im + SMOOTHING)
        return jnp.concatenate([(far_re * factor).astype(BF16), (far_im * factor).astype(BF16)], axis=0)

    def step(number, carried):
        duos = [(number * GROUP + 2 * duo, number * GROUP + 2 * duo + 1) for duo in range(GROUP // 2)]
        waves = [[wave_of(member) for member in two] for two in duos]
        halves = []
        for both in waves:
            stacked = jnp.concatenate(
                [jnp.concatenate([re.astype(BF16), im.astype(BF16)], axis=1) for re, im in both], axis=0
            )
            halves.append(jnp.dot(stacked, minus_ref[...], preferred_element_type=F32).astype(BF16))
        fars = [jnp.dot(plus_ref[...], by_lane(half), preferred_element_type=F32) for half in halves]
        resids = [residual(far, two) for far, two in zip(fars, duos)]
        backs = [jnp.dot(minus_ref[...], resid, preferred_element_type=F32).astype(BF16) for resid in resids]
        nears = [jnp.dot(by_lane(back), plus_ref[...], preferred_element_type=F32) for back in backs]
        for near, two, both in zip(nears, duos, waves):
            for slot, member in enumerate(two):
                wave_re, wave_im = both[slot]
                cut = slice(slot * side, (slot + 1) * side)
                add(member, near[cut, LANES:] * wave_re - near[cut, :LANES] * wave_im)
        return carried

    lax.fori_loop(0, frames // GROUP, step, 0)
    for p in range(pairs):
        for hi in range(2):
            for b in range(own):
                out_ref[p, hi * own + b] = acc[p + hi * pairs, b].astype(WIRE).reshape(out_ref.shape[2:])
        out_ref[p, 2 * own] = halo_join(acc[p, own], acc[p + pairs, own]).astype(WIRE).reshape(out_ref.shape[2:])


def complex_tables(length):
    indices = np.arange(length)
    phases = (indices[:, None] * indices[None, :] % length) * (2.0 * math.pi / length)
    cosine, sine = np.cos(phases), np.sin(phases)
    minus = np.block([[cosine, -sine], [sine, cosine]])
    plus = np.block([[cosine, sine], [-sine, cosine]]) / length
    return jnp.asarray(minus, BF16), jnp.asarray(plus, BF16)


def frame_gradients(owner, shift, cosine, sine, probe, measured, own, chips):
    pairs, waves, rows, unused = cosine.shape
    smem = pl.BlockSpec(memory_space=pltpu.SMEM)
    vmem = pl.BlockSpec(memory_space=pltpu.VMEM)
    return pl.pallas_call(
        functools.partial(frame_kernel, own),
        out_shape=jax.ShapeDtypeStruct((pairs, waves - 1, chips, rows // chips, LANES), WIRE),
        in_specs=[smem, smem] + [vmem] * 6,
        out_specs=vmem,
        scratch_shapes=[pltpu.VMEM((2 * pairs, own + 1, rows, LANES), F32)],
        compiler_params=pltpu.CompilerParams(vmem_limit_bytes=48 * 1024 * 1024),
        name="frames",
    )(owner, shift, cosine, sine, probe, measured, *complex_tables(LANES))


def backproject_kernel(slices, blocks, beams, lhs_ref, ker_ref, part_ref, out_hbm, out_ref, sems):
    groups = beams // 8
    width = 8 * HALF
    half_rows = slices * blocks
    left = lane_ids((half_rows, LANES)) < HALF

    def copy_out(group):
        return pltpu.make_async_copy(out_ref.at[:, group], out_hbm.at[:, group], sems.at[group])

    def step(group, carried):
        start = pl.multiple_of(group * width, width)
        span = pl.ds(start, width)
        result = part_ref[:, span] + jnp.dot(lhs_ref[...], ker_ref[:, span], preferred_element_type=F32)
        for pair in range(4):
            cols = slice(pair * LANES, (pair + 1) * LANES)
            lower, upper = result[:half_rows, cols], result[half_rows:, cols]
            crossed = pltpu.roll(jnp.where(left, upper, lower), HALF, 1)
            first = jnp.where(left, lower, crossed)
            second = jnp.where(left, crossed, upper)
            for s in range(slices):
                cut = slice(s * blocks, (s + 1) * blocks)
                out_ref[s, group, pl.ds(2 * pair, blocks, stride=8), :] = first[cut]
                out_ref[s, group, pl.ds(2 * pair + 1, blocks, stride=8), :] = second[cut]
        copy_out(group).start()
        return carried

    lax.fori_loop(0, groups, step, 0, unroll=True)

    def finish(group, carried):
        copy_out(group).wait()
        return carried

    lax.fori_loop(0, groups, finish, 0)


def backproject(lhs, kernels, partial_sum, slices, beams, blocks):
    groups = beams // 8
    shape = (slices, groups, blocks * 8, LANES)
    result = pl.pallas_call(
        functools.partial(backproject_kernel, slices, blocks, beams),
        out_shape=jax.ShapeDtypeStruct(shape, F32),
        in_specs=[pl.BlockSpec(memory_space=pltpu.VMEM)] * 3,
        out_specs=pl.BlockSpec(memory_space=pltpu.HBM),
        scratch_shapes=[pltpu.VMEM(shape, F32), pltpu.SemaphoreType.DMA((groups,))],
        compiler_params=pltpu.CompilerParams(vmem_limit_bytes=32 * 1024 * 1024),
        name="backproject",
    )(lhs, kernels, partial_sum)
    result = result.reshape(slices, groups, blocks, 8, LANES).transpose(0, 1, 3, 2, 4)
    return result.reshape(slices, beams, blocks * LANES)


def body(volume, shears, tile_shift, illumination, measured, frame_owner, frame_shift):
    tiles, slabs = lax.axis_size("tile"), lax.axis_size("slab")
    slices, beams, width = volume.shape
    blocks = width // LANES
    offsets = tile_shift.reshape(-1)
    owner = frame_owner.reshape(-1)
    cosine, sine = phase_waves(shears, offsets, volume, tiles, slabs)
    grads = frame_gradients(owner, frame_shift, cosine, sine, illumination, measured, blocks // tiles, slabs // 2)
    lhs, kernels, partial_sum = back_operands(shears, offsets, grads, tiles, slabs, blocks, beams)
    return backproject(lhs, kernels, partial_sum, slices, beams, blocks)


def solution(mesh):
    in_specs = (
        P("slab", "tile", None),
        P(),
        P(None, "tile"),
        P(),
        P(("slab", "tile"), None, None),
        P(("slab", "tile"), None),
        P(("slab", "tile")),
    )
    out_specs = P("slab", "tile", None)
    return jax.shard_map(body, mesh=mesh, in_specs=in_specs, out_specs=out_specs, check_vma=False)
```
